256 devices in a mesh: cuts: 8 (over z_lo, core), tile: 2 (over z_hi), probe: 16 (over x, y).
Axes of the slice: x: 4, y: 4, z: 8 (z_hi: 2, z_lo: 4; z = z_hi * 4 + z_lo), core: 2. Of those that a mesh axis runs over, the one named last changes fastest.
Arguments:
- probe_wave: bfloat16 [2, 512, 512], replicated, may hold values from -6 to 6
- fresnel_rows: bfloat16 [2, 512, 512], replicated, may hold values from -0.1875 to 0.1875
- fresnel_cols: bfloat16 [2, 512, 512], replicated, may hold values from -0.1875 to 0.1875
- object_slices: float32 [8, 2, 1024, 768], P('cuts', None, 'tile'), may hold values from -1 to 1.9, as said below
- offsets: int32 [2, 32, 2], P('tile', 'probe'), may hold values from 0 to 256
- measured: float32 [2, 32, 512, 512], P('tile', 'probe'), may hold values from 0.2 to 2
Outputs:
- updated_object: float32 [8, 2, 1024, 768], P('cuts', None, ('tile', 'probe'))
The draws below stay inside these ranges and needn't reach their ends.
Inputs may be any that keep to these rules, and one draw needn't show every extreme that they name: `object_slices`: real and imaginary parts of each slice's transmission.
All inputs are finite; a program needn't handle non-finite values.
Results may differ from the reference program's by a relative error of at most 0.02.
Values may be sent and summed in bfloat16 or wider, within the bound.
A program may use at most 128 MiB of HBM per device.

```python
import jax
import jax.numpy as jnp
from jax import lax

WINDOW = 512
MARGIN = 128
OWN_ROWS = 512
COLS = 768
ROWS = 1024
SLICES = 8
POSITIONS = 32
N_TILE = 2


def draw_object_slices(key, part):
    dimensions = (SLICES, 2, ROWS, COLS)
    jitter = jnp.clip(0.25 * jax.random.normal(key, dimensions, jnp.float32), -1.0, 1.0)
    center_value = jnp.array([0.9, 0.0], jnp.float32).reshape(1, 2, 1, 1)
    return center_value + jitter


def draw_offsets(key, part):
    row_key = jax.random.fold_in(key, 11)
    col_key = jax.random.fold_in(key, 23)
    row_most = OWN_ROWS + 2 * MARGIN - WINDOW
    col_most = 2 * MARGIN
    row_part = jax.random.randint(row_key, (N_TILE, POSITIONS), 0, row_most + 1, jnp.int32)
    col_part = jax.random.randint(col_key, (N_TILE, POSITIONS), 0, col_most + 1, jnp.int32)
    row_part = row_part.at[:, 0].set(row_most).at[:, 1].set(0)
    col_part = col_part.at[:, 0].set(col_most)
    return jnp.stack([row_part, col_part], axis=2).astype(jnp.int32)


def levels(stream_key, shape, shards, least, top_value):
    def one(dim, parts):
        heights = jax.random.uniform(jax.random.fold_in(jax.random.fold_in(stream_key, 6), dim), (parts,), jnp.float32, least / len(shards), top_value / len(shards))
        return jnp.repeat(jnp.exp(heights), shape[dim] // parts).reshape((-1,) + (1,) * (len(shape) - dim - 1))

    level = one(*shards[0])
    for cut in shards[1:]:
        level = level * one(*cut)
    return level


def gaussian(own_key, shape, width, limit, kind=jnp.bfloat16):
    values = jax.random.normal(own_key, shape, jnp.float32) * width
    return jnp.minimum(jnp.maximum(values, -limit), limit).astype(kind)


def setup_inputs(seed: int = 0) -> dict:
    seeds = jax.random.split(jax.random.key(seed), 7)
    probe_wave = gaussian(seeds[0], (2, WINDOW, WINDOW), 1.0, 6.0)
    fresnel_rows = gaussian(seeds[1], (2, WINDOW, WINDOW), (2 * WINDOW) ** -0.5, 0.1875)
    fresnel_cols = gaussian(seeds[2], (2, WINDOW, WINDOW), (2 * WINDOW) ** -0.5, 0.1875)
    object_slices = draw_object_slices(jax.random.fold_in(seeds[6], 71), 0)
    offsets = draw_offsets(jax.random.fold_in(seeds[6], 71), 0)
    measured = jnp.clip(0.2 + 1.8 * jax.random.uniform(seeds[5], (N_TILE, POSITIONS, WINDOW, WINDOW), jnp.float32) ** levels(seeds[5], (N_TILE, POSITIONS, WINDOW, WINDOW), ((0, 2), (1, 16)), -0.2, 0.2), 0.2, 2.0)
    return {"probe_wave": probe_wave, "fresnel_rows": fresnel_rows, "fresnel_cols": fresnel_cols, "object_slices": object_slices, "offsets": offsets, "measured": measured}


def right_product(wave_part, matrix):
    return jnp.einsum('mij,jk->mik', wave_part.astype(jnp.float32), matrix.astype(jnp.float32))

def left_product(matrix, wave_part):
    return jnp.einsum('ij,mjk->mik', matrix.astype(jnp.float32), wave_part.astype(jnp.float32))

def propagate(wave, rows_matrix, cols_matrix):
    real_in, imag_in = (wave[:, 0], wave[:, 1])
    col_real, col_imag = (cols_matrix[0].T, cols_matrix[1].T)
    mid_real = right_product(real_in, col_real) - right_product(imag_in, col_imag)
    mid_imag = right_product(real_in, col_imag) + right_product(imag_in, col_real)
    middle = jnp.stack([mid_real, mid_imag], axis=1).astype(jnp.bfloat16)
    row_real, row_imag = (rows_matrix[0], rows_matrix[1])
    out_real = left_product(row_real, middle[:, 0]) - left_product(row_imag, middle[:, 1])
    out_imag = left_product(row_imag, middle[:, 0]) + left_product(row_real, middle[:, 1])
    return jnp.stack([out_real, out_imag], axis=1).astype(jnp.bfloat16)

def adjoint(wave, rows_matrix, cols_matrix):
    real_in, imag_in = (wave[:, 0], wave[:, 1])
    col_real, col_imag = (cols_matrix[0], cols_matrix[1])
    mid_real = right_product(real_in, col_real) + right_product(imag_in, col_imag)
    mid_imag = right_product(imag_in, col_real) - right_product(real_in, col_imag)
    middle = jnp.stack([mid_real, mid_imag], axis=1).astype(jnp.bfloat16)
    row_real, row_imag = (rows_matrix[0].T, rows_matrix[1].T)
    out_real = left_product(row_real, middle[:, 0]) + left_product(row_imag, middle[:, 1])
    out_imag = left_product(row_real, middle[:, 1]) - left_product(row_imag, middle[:, 0])
    return jnp.stack([out_real, out_imag], axis=1).astype(jnp.bfloat16)

def complex_mul(left_side, right_side):
    return jnp.stack([left_side[:, 0] * right_side[:, 0] - left_side[:, 1] * right_side[:, 1], left_side[:, 0] * right_side[:, 1] + left_side[:, 1] * right_side[:, 0]], axis=1)

def conj_mul(left_side, right_side):
    return jnp.stack([left_side[:, 0] * right_side[:, 0] + left_side[:, 1] * right_side[:, 1], left_side[:, 0] * right_side[:, 1] - left_side[:, 1] * right_side[:, 0]], axis=1)

def reference(probe_wave, fresnel_rows, fresnel_cols, object_slices, offsets, measured):
    transmission = object_slices.astype(jnp.bfloat16)
    padded = jnp.concatenate([transmission[:, :, ROWS - MARGIN:], transmission, transmission[:, :, :MARGIN]], axis=2)
    tile_ids = jnp.arange(N_TILE, dtype=jnp.int32)
    row_starts = (tile_ids[:, None] * OWN_ROWS + offsets[:, :, 0]).reshape(-1).astype(jnp.int32)
    col_starts = offsets[:, :, 1].reshape(-1).astype(jnp.int32)
    total = N_TILE * POSITIONS

    def windows_of(slab):

        def cut_window(row_start, col_start):
            return lax.dynamic_slice(slab, (jnp.int32(0), row_start, col_start), (2, WINDOW, WINDOW))
        return jax.vmap(cut_window)(row_starts, col_starts)
    current = jnp.broadcast_to(probe_wave, (total, 2, WINDOW, WINDOW))
    stored_waves = []
    for slice_index in range(SLICES):
        stored_waves.append(current)
        windows = windows_of(padded[slice_index]).astype(jnp.float32)
        exits = complex_mul(current.astype(jnp.float32), windows).astype(jnp.bfloat16)
        current = propagate(exits, fresnel_rows, fresnel_cols)
    psi_final = current.astype(jnp.float32)
    amplitude = measured.reshape(total, WINDOW, WINDOW)
    factor = 1.0 - amplitude / jnp.sqrt(psi_final[:, 0] ** 2 + psi_final[:, 1] ** 2 + 1.0)
    cotangent = (psi_final * factor[:, None]).astype(jnp.bfloat16)
    results = [None] * SLICES
    for slice_index in reversed(range(SLICES)):
        backed = adjoint(cotangent, fresnel_rows, fresnel_cols).astype(jnp.float32)
        windows = windows_of(padded[slice_index]).astype(jnp.float32)
        incoming = stored_waves[slice_index].astype(jnp.float32)
        gradient_term = conj_mul(incoming, backed)
        intensity = incoming[:, 0] ** 2 + incoming[:, 1] ** 2
        cotangent = conj_mul(windows, backed).astype(jnp.bfloat16)
        pieces = jnp.concatenate([gradient_term, intensity[:, None]], axis=1)

        def add_piece(position, accum_grid):
            row_start = row_starts[position]
            col_start = col_starts[position]
            anchor = (jnp.int32(0), row_start, col_start)
            current_block = lax.dynamic_slice(accum_grid, anchor, (3, WINDOW, WINDOW))
            return lax.dynamic_update_slice(accum_grid, current_block + pieces[position], anchor)
        accum_grid = jnp.zeros((3, ROWS + 2 * MARGIN, COLS), jnp.float32)
        accum_grid = lax.fori_loop(0, total, add_piece, accum_grid)
        inside = accum_grid[:, MARGIN:MARGIN + ROWS]
        inside = inside.at[:, :MARGIN].add(accum_grid[:, MARGIN + ROWS:])
        inside = inside.at[:, ROWS - MARGIN:].add(accum_grid[:, :MARGIN])
        results[slice_index] = object_slices[slice_index] - inside[:2] / (inside[2] + 1.0)
    return jnp.stack(results, axis=0)
```

```python
import jax
import jax.numpy as jnp
from jax import lax
from jax.experimental import pallas as pl
from jax.experimental.pallas import tpu as pltpu
from jax.sharding import Mesh
from jax.sharding import PartitionSpec as P

MARGIN = 128
LANES = 128
SUB = 8
PROBE = ("probe_0", "probe_1")
TILE_PROBE = ("tile", "probe_0", "probe_1")
MESH_ID = pl.DeviceIdType.MESH
BF = jnp.bfloat16
F32 = jnp.float32
VMEM = pltpu.VMEM


def cut_kernel(starts, slab, out):
    positions, chunks, size, _ = out.shape
    width = slab.shape[2]
    block = 64
    for position in range(positions):
        row = starts[position, 0]
        col = starts[position, 1]
        shift = lax.rem(width - col, width)
        base = row // SUB * SUB
        drop = lax.rem(block + SUB - lax.rem(row, SUB), block + SUB)

        def rows(step, carry):
            at = pl.multiple_of(step * block, block)
            for part in range(2):
                values = slab[part, pl.ds(pl.multiple_of(base + at, SUB), block + SUB), :]
                turned = pltpu.roll(values, shift, 1)[:, :size]
                turned = pltpu.roll(turned, drop, 0)[:block]
                for chunk in range(chunks):
                    out[position, chunk, pl.ds(at, block), part * LANES : (part + 1) * LANES] = turned[
                        :, chunk * LANES : (chunk + 1) * LANES
                    ].astype(BF)
            return carry

        lax.fori_loop(0, size // block, rows, 0)


def place_kernel(starts, grads, lights, out, total):
    positions, chunks, size, _ = grads.shape
    blocks, _, each, width = out.shape
    block = 64
    total[...] = jnp.zeros_like(total)
    for position in range(positions):
        row = starts[position, 0]
        col = starts[position, 1]
        base = row // SUB * SUB
        drop = lax.rem(row, SUB)

        def rows(step, carry):
            at = pl.multiple_of(step * block, block)
            for part in range(3):
                pieces = []
                for chunk in range(chunks):
                    if part < 2:
                        piece = grads[position, chunk, pl.ds(at, block), part * LANES : (part + 1) * LANES]
                    else:
                        piece = lights[position, chunk, pl.ds(at, block), :]
                    pieces.append(piece.astype(F32))
                lines = jnp.concatenate(pieces, axis=1)
                lines = pltpu.roll(jnp.concatenate([lines, jnp.zeros((SUB, size), F32)], axis=0), drop, 0)
                lines = jnp.concatenate([lines, jnp.zeros((block + SUB, width - size), F32)], axis=1)
                turned = pltpu.roll(lines, col, 1)
                where = pl.ds(pl.multiple_of(base + at, SUB), block + SUB)
                total[part, where, :] = total[part, where, :] + turned
            return carry

        lax.fori_loop(0, size // block, rows, 0)
    own = 2 * each // 3
    edge = each - own
    half = blocks // 2
    for index in range(blocks):
        first = MARGIN + index * own
        out[index, :, 0:own, :] = total[:, first : first + own, :].astype(BF)
        first = index * edge
        if index >= half:
            first += blocks * own
        out[index, :, own:each, :] = total[:, first : first + edge, :].astype(BF)


def chain_kernel(
    probe, windows, forward_cols, adjoint_cols, forward_rows, adjoint_rows, measured,
    grads, lights,
    waves, cots, wave_out, cot_out, total, middle, backs,
    send_f, recv_f, send_b, recv_b,
):
    me = lax.axis_index("cuts")
    count = lax.axis_size("cuts")
    last = count - 1
    right = lax.rem(me + 1, count)
    left = lax.rem(me + count - 1, count)
    positions, chunks, size, pair = windows.shape
    half = pair // 2

    barrier = pltpu.get_barrier_semaphore()
    for other in (left, right):
        pl.semaphore_signal(barrier, inc=1, device_id={"cuts": other}, device_id_type=MESH_ID)

    total[...] = jnp.zeros_like(total)

    @pl.when(me == 0)
    def _():
        for position in range(positions):
            waves[position] = probe[...]

    pl.semaphore_wait(barrier, 2)

    def forward_copy(position, chunk):
        return pltpu.make_async_remote_copy(
            src_ref=wave_out.at[position, chunk],
            dst_ref=waves.at[position, chunk],
            send_sem=send_f.at[position, chunk],
            recv_sem=recv_f.at[position, chunk],
            device_id={"cuts": right},
            device_id_type=MESH_ID,
        )

    def adjoint_copy(position, chunk):
        return pltpu.make_async_remote_copy(
            src_ref=cot_out.at[position, chunk],
            dst_ref=cots.at[position, chunk],
            send_sem=send_b.at[position, chunk],
            recv_sem=recv_b.at[position, chunk],
            device_id={"cuts": left},
            device_id_type=MESH_ID,
        )

    def parts_of(value):
        value = value.astype(F32)
        return value[:, :half], value[:, half:]

    def both(real, imag):
        return jnp.concatenate([real, imag], axis=1)

    def to_middle():
        for chunk in range(chunks):
            columns = slice(chunk * pair, (chunk + 1) * pair)
            middle[chunk] = total[:, columns].astype(BF)
        total[...] = jnp.zeros_like(total)

    def forward(position):
        def gather(chunk, carry):
            @pl.when(me > 0)
            def _():
                forward_copy(position, chunk).wait_recv()

            wave_r, wave_i = parts_of(waves[position, chunk])
            win_r, win_i = parts_of(windows[position, chunk])
            out = both(wave_r * win_r - wave_i * win_i, wave_r * win_i + wave_i * win_r).astype(BF)
            total[...] += jnp.dot(out, forward_cols[chunk], preferred_element_type=F32)
            return carry

        lax.fori_loop(0, chunks, gather, 0)
        to_middle()

        def produce(chunk, carry):
            result = jnp.dot(forward_rows[...], middle[chunk], preferred_element_type=F32)
            real = result[:size, :half] - result[size:, half:]
            imag = result[size:, :half] + result[:size, half:]
            wave_out[position, chunk] = both(real, imag).astype(BF)

            @pl.when(me < last)
            def _():
                forward_copy(position, chunk).start()

            @pl.when(me == last)
            def _():
                psi_r, psi_i = parts_of(wave_out[position, chunk])
                amplitude = measured[position, chunk]
                factor = 1.0 - amplitude * lax.rsqrt(psi_r * psi_r + psi_i * psi_i + 1.0)
                cots[position, chunk] = both(psi_r * factor, psi_i * factor).astype(BF)

            return carry

        lax.fori_loop(0, chunks, produce, 0)

        def brighten(chunk, carry):
            wave_r, wave_i = parts_of(waves[position, chunk])
            lights[position, chunk] = (wave_r * wave_r + wave_i * wave_i).astype(BF)
            return carry

        lax.fori_loop(0, chunks, brighten, 0)

    def adjoint(position):
        def gather(chunk, carry):
            @pl.when(me < last)
            def _():
                adjoint_copy(position, chunk).wait_recv()

            total[...] += jnp.dot(cots[position, chunk], adjoint_cols[chunk], preferred_element_type=F32)
            return carry

        lax.fori_loop(0, chunks, gather, 0)
        to_middle()

        def produce(chunk, carry):
            result = jnp.dot(adjoint_rows[...], middle[chunk], preferred_element_type=F32)
            real = result[:size, :half] + result[size:, half:]
            imag = result[:size, half:] - result[size:, :half]
            back = both(real, imag).astype(BF)
            backs[chunk] = back

            @pl.when(me > 0)
            def _():
                back_r, back_i = parts_of(back)
                win_r, win_i = parts_of(windows[position, chunk])
                cot_out[position, chunk] = both(
                    win_r * back_r + win_i * back_i, win_r * back_i - win_i * back_r
                ).astype(BF)
                adjoint_copy(position, chunk).start()

            return carry

        lax.fori_loop(0, chunks, produce, 0)

        def grade(chunk, carry):
            wave_r, wave_i = parts_of(waves[position, chunk])
            back_r, back_i = parts_of(backs[chunk])
            grads[position, chunk] = both(
                wave_r * back_r + wave_i * back_i, wave_r * back_i - wave_i * back_r
            ).astype(BF)
            return carry

        lax.fori_loop(0, chunks, grade, 0)

    late = me // (count - 2)

    def phase(step, carry):
        is_back = late * (step % positions) + (1 - late) * (step // positions)
        position = late * (step // positions) + (1 - late) * (step % positions)

        @pl.when(is_back == 0)
        def _():
            forward(position)

        @pl.when(is_back == 1)
        def _():
            adjoint(position)

        return carry

    lax.fori_loop(0, 2 * positions, phase, 0)

    def finish(index, carry):
        position = index // chunks
        chunk = index % chunks

        @pl.when(me < last)
        def _():
            forward_copy(position, chunk).wait_send()

        @pl.when(me > 0)
        def _():
            adjoint_copy(position, chunk).wait_send()

        return carry

    lax.fori_loop(0, positions * chunks, finish, 0)


def column_blocks(matrix, chunks):
    _, _, depth, width = matrix.shape
    cut = matrix.reshape(2, 2, chunks, depth // chunks, chunks, width // chunks)
    return cut.transpose(2, 0, 3, 4, 1, 5).reshape(chunks, 2 * depth // chunks, 2 * width)


def in_vmem(count):
    return [pl.BlockSpec(memory_space=pltpu.VMEM)] * count


def shards(probe_wave, fresnel_rows, fresnel_cols, object_slices, offsets, measured):
    owned = object_slices[0]
    starts = offsets[0]
    size = probe_wave.shape[1]
    positions = starts.shape[0]
    rows, width = owned.shape[1:]
    chunks = size // LANES
    pair = 2 * LANES
    probe_index = lax.axis_index(PROBE)
    probe_count = lax.axis_size(PROBE)

    transmission = owned.astype(BF)
    edges = jnp.concatenate([transmission[:, rows - MARGIN :], transmission[:, :MARGIN]], axis=1)
    share = edges.shape[1] // probe_count
    mine = lax.dynamic_slice_in_dim(edges, probe_index * share, share, 1)
    swapped = lax.ppermute(mine, "tile", [(0, 1), (1, 0)])
    theirs = lax.all_gather(swapped, PROBE, axis=1, tiled=True)
    slab = jnp.concatenate([theirs[:, :MARGIN], transmission, theirs[:, MARGIN:]], axis=1).astype(F32)
    slab = jnp.pad(slab, ((0, 0), (0, SUB), (0, 0)))

    windows = pl.pallas_call(
        cut_kernel,
        out_shape=jax.ShapeDtypeStruct((positions, chunks, size, pair), BF),
        in_specs=[pl.BlockSpec(memory_space=pltpu.SMEM)] + in_vmem(1),
        out_specs=pl.BlockSpec(memory_space=pltpu.VMEM),
        name="cut",
    )(starts, slab)

    col_r, col_i = fresnel_cols[0], fresnel_cols[1]
    forward_cols = column_blocks(jnp.stack([jnp.stack([col_r.T, col_i.T]), jnp.stack([-col_i.T, col_r.T])]), chunks)
    adjoint_cols = column_blocks(jnp.stack([jnp.stack([col_r, -col_i]), jnp.stack([col_i, col_r])]), chunks)
    forward_rows = fresnel_rows.reshape(2 * size, size)
    adjoint_rows = fresnel_rows.swapaxes(1, 2).reshape(2 * size, size)
    probe = probe_wave.reshape(2, size, chunks, LANES).transpose(2, 1, 0, 3).reshape(chunks, size, pair)
    amplitude = measured[0].reshape(positions, size, chunks, LANES).transpose(0, 2, 1, 3)

    wave_stack = pltpu.VMEM((positions, chunks, size, pair), BF)
    grads, lights = pl.pallas_call(
        chain_kernel,
        out_shape=[
            jax.ShapeDtypeStruct((positions, chunks, size, pair), BF),
            jax.ShapeDtypeStruct((positions, chunks, size, LANES), BF),
        ],
        in_specs=in_vmem(7),
        out_specs=in_vmem(2),
        scratch_shapes=[
            wave_stack,
            wave_stack,
            wave_stack,
            wave_stack,
            pltpu.VMEM((size, 2 * size), F32),
            pltpu.VMEM((chunks, size, pair), BF),
            pltpu.VMEM((chunks, size, pair), BF),
            pltpu.SemaphoreType.DMA((positions, chunks)),
            pltpu.SemaphoreType.DMA((positions, chunks)),
            pltpu.SemaphoreType.DMA((positions, chunks)),
            pltpu.SemaphoreType.DMA((positions, chunks)),
        ],
        compiler_params=pltpu.CompilerParams(collective_id=0, has_side_effects=True, vmem_limit_bytes=60 * 2**20),
        name="chain",
    )(probe, windows, forward_cols, adjoint_cols, forward_rows, adjoint_rows, amplitude)

    own = rows // probe_count
    edge = 2 * MARGIN // probe_count
    grid = pl.pallas_call(
        place_kernel,
        out_shape=jax.ShapeDtypeStruct((probe_count, 3, own + edge, width), BF),
        in_specs=[pl.BlockSpec(memory_space=pltpu.SMEM)] + in_vmem(2),
        out_specs=pl.BlockSpec(memory_space=pltpu.VMEM),
        scratch_shapes=[pltpu.VMEM((3, rows + 2 * MARGIN + SUB, width), F32)],
        name="place",
    )(starts, grads, lights)

    summed = grid
    for axis in PROBE:
        summed = lax.psum_scatter(summed, axis, scatter_dimension=0, tiled=True)
    summed = summed[0]
    inside = summed[:, :own].astype(F32)
    margin = summed[:, own:]
    per_own = own // edge
    half = probe_count // 2
    received = []
    for which in range(per_own):
        pairs = []
        for tile in range(2):
            for index in range(which, probe_count, per_own):
                if index < half:
                    target = probe_count - half // per_own + index // per_own
                else:
                    target = (index - half) // per_own
                pairs.append((tile * probe_count + index, (1 - tile) * probe_count + target))
        received.append(lax.ppermute(margin, TILE_PROBE, pairs))
    full = inside + jnp.concatenate(received, axis=1).astype(F32)
    own_part = lax.dynamic_slice_in_dim(owned, probe_index * own, own, 1)
    updated = own_part - full[:2] / (full[2] + 1.0)
    return updated[None]


def solution(mesh):
    split = Mesh(
        mesh.devices.reshape(mesh.shape["cuts"], mesh.shape["tile"], 4, 4),
        ("cuts", "tile", "probe_0", "probe_1"),
    )
    return jax.shard_map(
        shards,
        mesh=split,
        in_specs=(
            P(),
            P(),
            P(),
            P("cuts", None, "tile", None),
            P("tile", PROBE, None),
            P("tile", PROBE, None, None),
        ),
        out_specs=P("cuts", None, TILE_PROBE, None),
        check_vma=False,
    )
```

```python
import jax
import jax.numpy as jnp
from jax import lax
from jax.experimental import pallas as pl
from jax.experimental.pallas import tpu as pltpu
from jax.sharding import Mesh
from jax.sharding import PartitionSpec as P

MARGIN = 128
LANES = 128
SUB = 8
PROBE = ("probe_0", "probe_1")
TILE_PROBE = ("tile", "probe_0", "probe_1")
MESH_ID = pl.DeviceIdType.MESH
BF = jnp.bfloat16
F32 = jnp.float32
VMEM = pltpu.VMEM


def edge_kernel(owned, out, mine, got, gathered, send_z, recv_z, send_sem, recv_sem):
    tile, x, y = lax.axis_index("tile"), lax.axis_index("probe_0"), lax.axis_index("probe_1")
    nx, ny = lax.axis_size("probe_0"), lax.axis_size("probe_1")
    count = nx * ny
    me = x * ny + y
    rows = owned.shape[1]
    share = mine.shape[1]
    half = count // 2
    mate = {"tile": 1 - tile}

    def peer(step):
        other = lax.rem(me + step, count)
        return {"probe_0": other // ny, "probe_1": lax.rem(other, ny)}

    barrier = pltpu.get_barrier_semaphore()
    pl.semaphore_signal(barrier, inc=1, device_id=mate, device_id_type=MESH_ID)
    for step in range(1, count):
        pl.semaphore_signal(barrier, inc=1, device_id=peer(step), device_id_type=MESH_ID)

    lower = me // half
    first = (1 - lower) * (rows - MARGIN + me * share) + lower * (me - half) * share
    mine[...] = owned[:, pl.ds(pl.multiple_of(first, share), share), :].astype(BF)
    pl.semaphore_wait(barrier, count)

    swap = pltpu.make_async_remote_copy(
        src_ref=mine, dst_ref=got, send_sem=send_z, recv_sem=recv_z, device_id=mate, device_id_type=MESH_ID
    )
    swap.start()
    swap.wait_recv()

    def share_copy(step):
        return pltpu.make_async_remote_copy(
            src_ref=got,
            dst_ref=gathered.at[me],
            send_sem=send_sem.at[step],
            recv_sem=recv_sem.at[me],
            device_id=peer(step),
            device_id_type=MESH_ID,
        )

    def arrival(step):
        sender = lax.rem(me + count - step, count)
        return pltpu.make_async_remote_copy(
            src_ref=got,
            dst_ref=gathered.at[sender],
            send_sem=send_sem.at[step],
            recv_sem=recv_sem.at[sender],
            device_id=peer(step),
            device_id_type=MESH_ID,
        )

    for step in range(1, count):
        share_copy(step).start()
    out[me] = got[...]
    for step in range(1, count):
        arrival(step).wait_recv()
        sender = lax.rem(me + count - step, count)
        out[sender] = gathered[sender]
    swap.wait_send()
    for step in range(1, count):
        share_copy(step).wait_send()


def cut_kernel(starts, owned, edges, out, slab):
    positions, chunks, size, _ = out.shape
    rows, width = owned.shape[1:]
    count, _, share, _ = edges.shape
    block = 64
    for index in range(count):
        first = index * share + (rows if index >= count // 2 else 0)
        slab[:, first : first + share, :] = edges[index].astype(F32)
    slab[:, MARGIN : MARGIN + rows, :] = owned[...].astype(BF).astype(F32)
    slab[:, rows + 2 * MARGIN :, :] = jnp.zeros((2, SUB, width), F32)
    for position in range(positions):
        row = starts[position, 0]
        col = starts[position, 1]
        shift = lax.rem(width - col, width)
        base = row // SUB * SUB
        drop = lax.rem(block + SUB - lax.rem(row, SUB), block + SUB)

        def lines(step, carry):
            at = pl.multiple_of(step * block, block)
            for part in range(2):
                values = slab[part, pl.ds(pl.multiple_of(base + at, SUB), block + SUB), :]
                turned = pltpu.roll(values, shift, 1)[:, :size]
                turned = pltpu.roll(turned, drop, 0)[:block]
                for chunk in range(chunks):
                    out[position, chunk, pl.ds(at, block), part * LANES : (part + 1) * LANES] = turned[
                        :, chunk * LANES : (chunk + 1) * LANES
                    ].astype(BF)
            return carry

        lax.fori_loop(0, size // block, lines, 0)


def place_kernel(starts, grads, lights, out, total):
    positions, chunks, size, _ = grads.shape
    _, nx, ny, each, width = out.shape
    ny //= 3
    width *= 2
    block = 64
    total[...] = jnp.zeros_like(total)
    for position in range(positions):
        row = starts[position, 0]
        col = starts[position, 1]
        base = row // SUB * SUB
        drop = lax.rem(row, SUB)

        def rows(step, carry):
            at = pl.multiple_of(step * block, block)
            for part in range(3):
                pieces = []
                for chunk in range(chunks):
                    if part < 2:
                        piece = grads[position, chunk, pl.ds(at, block), part * LANES : (part + 1) * LANES]
                    else:
                        piece = lights[position, chunk, pl.ds(at, block), :]
                    pieces.append(piece.astype(F32))
                lines = jnp.concatenate(pieces, axis=1)
                lines = pltpu.roll(jnp.concatenate([lines, jnp.zeros((SUB, size), F32)], axis=0), drop, 0)
                lines = jnp.concatenate([lines, jnp.zeros((block + SUB, width - size), F32)], axis=1)
                turned = pltpu.roll(lines, col, 1)
                where = pl.ds(pl.multiple_of(base + at, SUB), block + SUB)
                total[part, where, :] = total[part, where, :] + turned
            return carry

        lax.fori_loop(0, size // block, rows, 0)
    own = 2 * each // 3
    edge = each - own
    for x in range(nx):
        for y in range(ny):
            index = x * ny + y
            first = MARGIN + index * own
            second = index * edge + (nx * ny * own if 2 * index >= nx * ny else 0)
            for side in range(2):
                major, minor = (x, y) if side == 0 else (y, x)
                lanes = slice(side * width // 2, (side + 1) * width // 2)
                place = slice(3 * minor, 3 * minor + 3)
                out[side, major, place, 0:own, :] = total[:, first : first + own, lanes].astype(BF)
                out[side, major, place, own:each, :] = total[:, second : second + edge, lanes].astype(BF)


def reduce_kernel(
    grid, owned, out,
    pre_up, pre_down, staged_up, staged_down, got_up, got_down, partial,
    pre_up2, pre_down2, staged_up2, staged_down2, got_up2, got_down2,
    final, extra, rows_here, send_sem, recv_sem, send_m, recv_m, local_sem,
):
    tile = lax.axis_index("tile")
    where = {"probe_0": lax.axis_index("probe_0"), "probe_1": lax.axis_index("probe_1")}
    sizes = {"probe_0": lax.axis_size("probe_0"), "probe_1": lax.axis_size("probe_1")}
    nx, ny = sizes["probe_0"], sizes["probe_1"]
    count = nx * ny
    me = where["probe_0"] * ny + where["probe_1"]
    each = grid.shape[3]
    own = 2 * each // 3
    edge = each - own
    lanes = grid.shape[4]
    half = count // 2
    order = (("probe_0", "probe_1"), ("probe_1", "probe_0"))

    def device(index):
        return {"tile": 1 - tile, "probe_0": index // ny, "probe_1": lax.rem(index, ny)}

    lower = me // half
    target = (1 - lower) * (count - half // 2 + me // 2) + lower * ((me - half) // 2)
    outer = where["probe_0"] // (nx - 1) + (nx - 1 - where["probe_0"]) // (nx - 1)
    source = where["probe_0"] // (nx - 1) * (2 * (me - count + half // 2)) + (
        nx - 1 - where["probe_0"]
    ) // (nx - 1) * (half + 2 * me)

    fetch = pltpu.make_async_copy(owned.at[:, pl.ds(pl.multiple_of(me * own, own), own), :], rows_here, local_sem)
    fetch.start()

    barrier = pltpu.get_barrier_semaphore()
    for axis in ("probe_0", "probe_1"):
        for step in (1, sizes[axis] - 1):
            other = {axis: lax.rem(where[axis] + step, sizes[axis])}
            pl.semaphore_signal(barrier, inc=1, device_id=other, device_id_type=MESH_ID)

    @pl.when(outer == 1)
    def _():
        for which in range(2):
            pl.semaphore_signal(barrier, inc=1, device_id=device(source + which), device_id_type=MESH_ID)

    pl.semaphore_wait(barrier, 5)

    def copies(stage, side, src, bufs):
        axis = order[side][stage]
        size = sizes[axis]
        here = where[axis]
        plus, minus = lax.rem(here + 1, size), lax.rem(here + size - 1, size)
        opposite = lax.rem(here + 2, size)
        up_pre, down_pre, up_staged, down_staged, up_got, down_got = bufs
        depth = src.shape[1]
        cut = (depth + 1) // 2
        low, high = pl.ds(0, cut), pl.ds(cut, depth - cut)

        def copy(index, source_ref, target_ref, to):
            return pltpu.make_async_remote_copy(
                src_ref=source_ref,
                dst_ref=target_ref,
                send_sem=send_sem.at[stage, side, index],
                recv_sem=recv_sem.at[stage, side, index],
                device_id={axis: to},
                device_id_type=MESH_ID,
            )

        return (
            copy(0, src.at[opposite, low], up_pre.at[side], plus),
            copy(1, src.at[opposite, high], down_pre.at[side], minus),
            copy(2, src.at[plus, high], up_got.at[side, high], plus),
            copy(3, src.at[minus, low], down_got.at[side, low], minus),
            copy(4, up_staged.at[side], up_got.at[side, low], plus),
            copy(5, down_staged.at[side], down_got.at[side, high], minus),
        ), (here, plus, minus, low, high)

    def begin(stage, side, src, bufs):
        made, _ = copies(stage, side, src, bufs)
        for index in range(4):
            made[index].start()

    def relay(stage, side, src, bufs):
        made, (_, plus, minus, low, high) = copies(stage, side, src, bufs)
        up_pre, down_pre, up_staged, down_staged, _, _ = bufs
        made[0].wait_recv()
        up_staged[side] = (up_pre[side].astype(F32) + src[plus, low].astype(F32)).astype(BF)
        made[4].start()
        made[1].wait_recv()
        down_staged[side] = (down_pre[side].astype(F32) + src[minus, high].astype(F32)).astype(BF)
        made[5].start()

    def settle(stage, side, src, bufs):
        made, (here, _, _, _, _) = copies(stage, side, src, bufs)
        for index in range(2, 6):
            made[index].wait_recv()
        up_got, down_got = bufs[4], bufs[5]
        return src[here].astype(F32) + up_got[side].astype(F32) + down_got[side].astype(F32)

    def drain(stage, side, src, bufs):
        for copy in copies(stage, side, src, bufs)[0]:
            copy.wait_send()

    one = (pre_up, pre_down, staged_up, staged_down, got_up, got_down)
    two = (pre_up2, pre_down2, staged_up2, staged_down2, got_up2, got_down2)
    for side in range(2):
        begin(0, side, grid.at[side], one)
    for side in range(2):
        relay(0, side, grid.at[side], one)
    for side in range(2):
        summed = settle(0, side, grid.at[side], one).astype(BF)
        for index in range(partial.shape[1]):
            partial[side, index] = summed[3 * index : 3 * index + 3]
        begin(1, side, partial.at[side], two)
    for side in range(2):
        relay(1, side, partial.at[side], two)
    for side in range(2):
        final[side] = settle(1, side, partial.at[side], two).astype(BF)

    def margin_copy(slot):
        return pltpu.make_async_remote_copy(
            src_ref=final.at[:, :, pl.ds(own, edge), :],
            dst_ref=extra.at[slot],
            send_sem=send_m,
            recv_sem=recv_m.at[slot],
            device_id=device(target),
            device_id_type=MESH_ID,
        )

    margin_copy(lax.rem(me, 2)).start()
    fetch.wait()

    @pl.when(outer == 0)
    def _():
        extra[...] = jnp.zeros_like(extra)

    @pl.when(outer == 1)
    def _():
        for slot in range(2):
            margin_copy(slot).wait_recv()

    for side in range(2):
        columns = slice(side * lanes, (side + 1) * lanes)
        for slot in range(2):
            lines = slice(slot * edge, (slot + 1) * edge)
            full = final[side, :, lines, :].astype(F32) + extra[slot, side].astype(F32)
            scale = 1.0 / (full[2] + 1.0)
            for part in range(2):
                out[part, lines, columns] = rows_here[part, lines, columns] - full[part] * scale
    margin_copy(lax.rem(me, 2)).wait_send()
    for side in range(2):
        drain(0, side, grid.at[side], one)
        drain(1, side, partial.at[side], two)


def chain_kernel(
    probe, windows, fresnel_cols, forward_rows, measured,
    grads, lights,
    forward_cols, adjoint_cols, adjoint_rows,
    waves, cots, wave_out, cot_out, total, middle, backs,
    send_f, recv_f, send_b, recv_b,
):
    me = lax.axis_index("cuts")
    count = lax.axis_size("cuts")
    last = count - 1
    right = lax.rem(me + 1, count)
    left = lax.rem(me + count - 1, count)
    positions, chunks, size, pair = windows.shape
    half = pair // 2

    barrier = pltpu.get_barrier_semaphore()
    for other in (left, right):
        pl.semaphore_signal(barrier, inc=1, device_id={"cuts": other}, device_id_type=MESH_ID)

    total[...] = jnp.zeros_like(total)
    first_half, second_half = slice(0, half), slice(half, pair)

    @pl.when(me == 0)
    def _():
        for position in range(positions):
            for chunk in range(chunks):
                lanes = slice(chunk * half, (chunk + 1) * half)
                waves[position, chunk, :, first_half] = probe[0, :, lanes]
                waves[position, chunk, :, second_half] = probe[1, :, lanes]

    def turned(value):
        return value.astype(F32).T.astype(BF)

    def prepare_forward(chunk, carry):
        lanes = pl.ds(pl.multiple_of(chunk * half, half), half)
        for other in range(chunks):
            lines = slice(other * half, (other + 1) * half)
            real, imag = turned(fresnel_cols[0, lines, lanes]), turned(fresnel_cols[1, lines, lanes])
            left_lanes = slice(other * pair, other * pair + half)
            right_lanes = slice(other * pair + half, (other + 1) * pair)
            forward_cols[chunk, first_half, left_lanes] = real
            forward_cols[chunk, first_half, right_lanes] = imag
            forward_cols[chunk, second_half, left_lanes] = -imag
            forward_cols[chunk, second_half, right_lanes] = real
        return carry

    lax.fori_loop(0, chunks, prepare_forward, 0)

    def prepare_adjoint(chunk, carry):
        lines = pl.ds(pl.multiple_of(chunk * half, half), half)
        for other in range(chunks):
            lanes = slice(other * half, (other + 1) * half)
            real, imag = fresnel_cols[0, lines, lanes], fresnel_cols[1, lines, lanes]
            left_lanes = slice(other * pair, other * pair + half)
            right_lanes = slice(other * pair + half, (other + 1) * pair)
            adjoint_cols[chunk, first_half, left_lanes] = real
            adjoint_cols[chunk, first_half, right_lanes] = -imag
            adjoint_cols[chunk, second_half, left_lanes] = imag
            adjoint_cols[chunk, second_half, right_lanes] = real
            for part in range(2):
                block = forward_rows[pl.ds(pl.multiple_of(part * size + chunk * half, half), half), lanes]
                adjoint_rows[part * size + other * half : part * size + (other + 1) * half, lines] = turned(block)
        return carry

    pl.semaphore_wait(barrier, 2)

    def forward_copy(position, chunk):
        return pltpu.make_async_remote_copy(
            src_ref=wave_out.at[position, chunk],
            dst_ref=waves.at[position, chunk],
            send_sem=send_f.at[position, chunk],
            recv_sem=recv_f.at[position, chunk],
            device_id={"cuts": right},
            device_id_type=MESH_ID,
        )

    def adjoint_copy(position, chunk):
        return pltpu.make_async_remote_copy(
            src_ref=cot_out.at[position, chunk],
            dst_ref=cots.at[position, chunk],
            send_sem=send_b.at[position, chunk],
            recv_sem=recv_b.at[position, chunk],
            device_id={"cuts": left},
            device_id_type=MESH_ID,
        )

    def parts_of(value):
        value = value.astype(F32)
        return value[:, :half], value[:, half:]

    def both(real, imag):
        return jnp.concatenate([real, imag], axis=1)

    def to_middle():
        for chunk in range(chunks):
            columns = slice(chunk * pair, (chunk + 1) * pair)
            middle[chunk] = total[:, columns].astype(BF)
        total[...] = jnp.zeros_like(total)

    def forward(position):
        def gather(chunk, carry):
            @pl.when(me > 0)
            def _():
                forward_copy(position, chunk).wait_recv()

            wave_r, wave_i = parts_of(waves[position, chunk])
            win_r, win_i = parts_of(windows[position, chunk])
            out = both(wave_r * win_r - wave_i * win_i, wave_r * win_i + wave_i * win_r).astype(BF)
            total[...] += jnp.dot(out, forward_cols[chunk], preferred_element_type=F32)
            return carry

        lax.fori_loop(0, chunks, gather, 0)
        to_middle()

        def produce(chunk, carry):
            result = jnp.dot(forward_rows[...], middle[chunk], preferred_element_type=F32)
            real = result[:size, :half] - result[size:, half:]
            imag = result[size:, :half] + result[:size, half:]
            wave_out[position, chunk] = both(real, imag).astype(BF)

            @pl.when(me < last)
            def _():
                forward_copy(position, chunk).start()

            @pl.when(me == last)
            def _():
                psi_r, psi_i = parts_of(wave_out[position, chunk])
                amplitude = measured[position, :, pl.ds(pl.multiple_of(chunk * half, half), half)]
                factor = 1.0 - amplitude * lax.rsqrt(psi_r * psi_r + psi_i * psi_i + 1.0)
                cots[position, chunk] = both(psi_r * factor, psi_i * factor).astype(BF)

            return carry

        lax.fori_loop(0, chunks, produce, 0)

        def brighten(chunk, carry):
            wave_r, wave_i = parts_of(waves[position, chunk])
            lights[position, chunk] = (wave_r * wave_r + wave_i * wave_i).astype(BF)
            return carry

        lax.fori_loop(0, chunks, brighten, 0)

    def adjoint(position):
        def gather(chunk, carry):
            @pl.when(me < last)
            def _():
                adjoint_copy(position, chunk).wait_recv()

            total[...] += jnp.dot(cots[position, chunk], adjoint_cols[chunk], preferred_element_type=F32)
            return carry

        lax.fori_loop(0, chunks, gather, 0)
        to_middle()

        def produce(chunk, carry):
            result = jnp.dot(adjoint_rows[...], middle[chunk], preferred_element_type=F32)
            real = result[:size, :half] + result[size:, half:]
            imag = result[:size, half:] - result[size:, :half]
            back = both(real, imag).astype(BF)
            backs[chunk] = back

            @pl.when(me > 0)
            def _():
                back_r, back_i = parts_of(back)
                win_r, win_i = parts_of(windows[position, chunk])
                cot_out[position, chunk] = both(
                    win_r * back_r + win_i * back_i, win_r * back_i - win_i * back_r
                ).astype(BF)
                adjoint_copy(position, chunk).start()

            return carry

        lax.fori_loop(0, chunks, produce, 0)

        def grade(chunk, carry):
            wave_r, wave_i = parts_of(waves[position, chunk])
            back_r, back_i = parts_of(backs[chunk])
            grads[position, chunk] = both(
                wave_r * back_r + wave_i * back_i, wave_r * back_i - wave_i * back_r
            ).astype(BF)
            return carry

        lax.fori_loop(0, chunks, grade, 0)

    late = me // (count - 2)

    def phase(step, carry):
        is_back = late * (step % positions) + (1 - late) * (step // positions)
        position = late * (step // positions) + (1 - late) * (step % positions)

        @pl.when(step == positions * (1 - late))
        def _():
            lax.fori_loop(0, chunks, prepare_adjoint, 0)

        @pl.when(is_back == 0)
        def _():
            forward(position)

        @pl.when(is_back == 1)
        def _():
            adjoint(position)

        return carry

    lax.fori_loop(0, 2 * positions, phase, 0)

    def finish(index, carry):
        position = index // chunks
        chunk = index % chunks

        @pl.when(me < last)
        def _():
            forward_copy(position, chunk).wait_send()

        @pl.when(me > 0)
        def _():
            adjoint_copy(position, chunk).wait_send()

        return carry

    lax.fori_loop(0, positions * chunks, finish, 0)


def in_vmem(count):
    return [pl.BlockSpec(memory_space=pltpu.VMEM)] * count


def in_smem():
    return [pl.BlockSpec(memory_space=pltpu.SMEM)]


def on_chip(limit, **more):
    return pltpu.CompilerParams(vmem_limit_bytes=limit * 2**20, **more)


def shards(probe_wave, fresnel_rows, fresnel_cols, object_slices, offsets, measured):
    owned = object_slices[0]
    starts = offsets[0]
    size = probe_wave.shape[1]
    positions = starts.shape[0]
    rows, width = owned.shape[1:]
    chunks = size // LANES
    pair = 2 * LANES
    nx, ny = lax.axis_size("probe_0"), lax.axis_size("probe_1")
    count = nx * ny
    share = 2 * MARGIN // count
    own = rows // count
    each = own + share
    dma = pltpu.SemaphoreType.DMA

    edges = pl.pallas_call(
        edge_kernel,
        out_shape=jax.ShapeDtypeStruct((count, 2, share, width), BF),
        in_specs=in_vmem(1),
        out_specs=pl.BlockSpec(memory_space=pltpu.VMEM),
        scratch_shapes=[
            VMEM((2, share, width), BF),
            VMEM((2, share, width), BF),
            VMEM((count, 2, share, width), BF),
            dma,
            dma,
            dma((count,)),
            dma((count,)),
        ],
        compiler_params=on_chip(24, collective_id=1, has_side_effects=True),
        name="edge",
    )(owned)

    windows = pl.pallas_call(
        cut_kernel,
        out_shape=jax.ShapeDtypeStruct((positions, chunks, size, pair), BF),
        in_specs=in_smem() + in_vmem(2),
        out_specs=pl.BlockSpec(memory_space=pltpu.VMEM),
        scratch_shapes=[VMEM((2, rows + 2 * MARGIN + SUB, width), F32)],
        compiler_params=on_chip(40),
        name="cut",
    )(starts, owned, edges)

    wave_stack = VMEM((positions, chunks, size, pair), BF)
    columns = VMEM((chunks, pair, 2 * size), BF)
    grads, lights = pl.pallas_call(
        chain_kernel,
        out_shape=[
            jax.ShapeDtypeStruct((positions, chunks, size, pair), BF),
            jax.ShapeDtypeStruct((positions, chunks, size, LANES), BF),
        ],
        in_specs=in_vmem(5),
        out_specs=in_vmem(2),
        scratch_shapes=[
            columns,
            columns,
            VMEM((2 * size, size), BF),
            wave_stack,
            wave_stack,
            wave_stack,
            wave_stack,
            VMEM((size, 2 * size), F32),
            VMEM((chunks, size, pair), BF),
            VMEM((chunks, size, pair), BF),
            dma((positions, chunks)),
            dma((positions, chunks)),
            dma((positions, chunks)),
            dma((positions, chunks)),
        ],
        compiler_params=on_chip(60, collective_id=0, has_side_effects=True),
        name="chain",
    )(probe_wave, windows, fresnel_cols, fresnel_rows.reshape(2 * size, size), measured[0])

    grid = pl.pallas_call(
        place_kernel,
        out_shape=jax.ShapeDtypeStruct((2, nx, 3 * ny, each, width // 2), BF),
        in_specs=in_smem() + in_vmem(2),
        out_specs=pl.BlockSpec(memory_space=pltpu.VMEM),
        scratch_shapes=[VMEM((3, rows + 2 * MARGIN + SUB, width), F32)],
        compiler_params=on_chip(40),
        name="place",
    )(starts, grads, lights)

    def slots(depth):
        return VMEM((2, depth, each, width // 2), BF)

    def ring(depth):
        cut = (depth + 1) // 2
        return [slots(cut), slots(depth - cut), slots(cut), slots(depth - cut), slots(depth), slots(depth)]

    updated = pl.pallas_call(
        reduce_kernel,
        out_shape=jax.ShapeDtypeStruct((2, own, width), F32),
        in_specs=in_vmem(1) + [pl.BlockSpec(memory_space=pl.ANY)],
        out_specs=pl.BlockSpec(memory_space=pltpu.VMEM),
        scratch_shapes=ring(3 * ny)
        + [VMEM((2, ny, 3, each, width // 2), BF)]
        + ring(3)
        + [
            slots(3),
            VMEM((2, 2, 3, share, width // 2), BF),
            VMEM((2, own, width), F32),
            dma((2, 2, 6)),
            dma((2, 2, 6)),
            dma,
            dma((2,)),
            dma,
        ],
        compiler_params=on_chip(40, collective_id=2, has_side_effects=True),
        name="reduce",
    )(grid, owned)
    return updated[None]


def solution(mesh):
    split = Mesh(
        mesh.devices.reshape(mesh.shape["cuts"], mesh.shape["tile"], 4, 4),
        ("cuts", "tile", "probe_0", "probe_1"),
    )
    return jax.shard_map(
        shards,
        mesh=split,
        in_specs=(
            P(),
            P(),
            P(),
            P("cuts", None, "tile", None),
            P("tile", PROBE, None),
            P("tile", PROBE, None, None),
        ),
        out_specs=P("cuts", None, TILE_PROBE, None),
        check_vma=False,
    )
```

```python
import jax
import jax.numpy as jnp
from jax import lax
from jax.experimental import pallas as pl
from jax.experimental.pallas import tpu as pltpu
from jax.sharding import Mesh
from jax.sharding import PartitionSpec as P

MARGIN = 128
LANES = 128
SUB = 8
HOSTED = 2
PROBE = ("probe_0", "probe_1")
TILE_PROBE = ("tile", "probe_0", "probe_1")
MESH_ID = pl.DeviceIdType.MESH
BF = jnp.bfloat16
F32 = jnp.float32
VMEM = pltpu.VMEM


def edge_kernel(owned, out, mine, got, gathered, send_z, recv_z, send_sem, recv_sem):
    tile, x, y = lax.axis_index("tile"), lax.axis_index("probe_0"), lax.axis_index("probe_1")
    nx, ny = lax.axis_size("probe_0"), lax.axis_size("probe_1")
    count = nx * ny
    me = x * ny + y
    rows = owned.shape[1]
    share = mine.shape[1]
    half = count // 2
    mate = {"tile": 1 - tile}

    def peer(step):
        other = lax.rem(me + step, count)
        return {"probe_0": other // ny, "probe_1": lax.rem(other, ny)}

    barrier = pltpu.get_barrier_semaphore()
    pl.semaphore_signal(barrier, inc=1, device_id=mate, device_id_type=MESH_ID)
    for step in range(1, count):
        pl.semaphore_signal(barrier, inc=1, device_id=peer(step), device_id_type=MESH_ID)

    lower = me // half
    first = (1 - lower) * (rows - MARGIN + me * share) + lower * (me - half) * share
    mine[...] = owned[:, pl.ds(pl.multiple_of(first, share), share), :].astype(BF)
    pl.semaphore_wait(barrier, count)

    swap = pltpu.make_async_remote_copy(
        src_ref=mine, dst_ref=got, send_sem=send_z, recv_sem=recv_z, device_id=mate, device_id_type=MESH_ID
    )
    swap.start()
    swap.wait_recv()

    def share_copy(step):
        return pltpu.make_async_remote_copy(
            src_ref=got,
            dst_ref=gathered.at[me],
            send_sem=send_sem.at[step],
            recv_sem=recv_sem.at[me],
            device_id=peer(step),
            device_id_type=MESH_ID,
        )

    def arrival(step):
        sender = lax.rem(me + count - step, count)
        return pltpu.make_async_remote_copy(
            src_ref=got,
            dst_ref=gathered.at[sender],
            send_sem=send_sem.at[step],
            recv_sem=recv_sem.at[sender],
            device_id=peer(step),
            device_id_type=MESH_ID,
        )

    for step in range(1, count):
        share_copy(step).start()
    out[me] = got[...]
    for step in range(1, count):
        arrival(step).wait_recv()
        sender = lax.rem(me + count - step, count)
        out[sender] = gathered[sender]
    swap.wait_send()
    for step in range(1, count):
        share_copy(step).wait_send()


def cut_kernel(starts, owned, edges, out, slab):
    positions, chunks, size, _ = out.shape
    rows, width = owned.shape[1:]
    count, _, share, _ = edges.shape
    block = 64
    for index in range(count):
        first = index * share + (rows if index >= count // 2 else 0)
        slab[:, first : first + share, :] = edges[index].astype(F32)
    slab[:, MARGIN : MARGIN + rows, :] = owned[...].astype(BF).astype(F32)
    slab[:, rows + 2 * MARGIN :, :] = jnp.zeros((2, SUB, width), F32)
    for position in range(positions):
        row = starts[position, 0]
        col = starts[position, 1]
        shift = lax.rem(width - col, width)
        base = row // SUB * SUB
        drop = lax.rem(block + SUB - lax.rem(row, SUB), block + SUB)

        def lines(step, carry):
            at = pl.multiple_of(step * block, block)
            for part in range(2):
                values = slab[part, pl.ds(pl.multiple_of(base + at, SUB), block + SUB), :]
                turned = pltpu.roll(values, shift, 1)[:, :size]
                turned = pltpu.roll(turned, drop, 0)[:block]
                for chunk in range(chunks):
                    out[position, chunk, pl.ds(at, block), part * LANES : (part + 1) * LANES] = turned[
                        :, chunk * LANES : (chunk + 1) * LANES
                    ].astype(BF)
            return carry

        lax.fori_loop(0, size // block, lines, 0)


def active_slots(me, count):
    return (1 + me // (count - 4)) * (1 - me // (count - 2))


def place_kernel(starts, grads, lights, out, total):
    _, positions, chunks, size, _ = grads.shape
    _, _, nx, ny, each, width = out.shape
    ny //= 3
    width *= 2
    block = 64
    own = 2 * each // 3
    edge = each - own

    def one_slot(slot, carry):
        total[...] = jnp.zeros_like(total)
        for position in range(positions):
            row = starts[position, 0]
            col = starts[position, 1]
            base = row // SUB * SUB
            drop = lax.rem(row, SUB)

            def rows(step, inner):
                at = pl.multiple_of(step * block, block)
                for part in range(3):
                    pieces = []
                    for chunk in range(chunks):
                        if part < 2:
                            piece = grads[slot, position, chunk, pl.ds(at, block), part * LANES : (part + 1) * LANES]
                        else:
                            piece = lights[slot, position, chunk, pl.ds(at, block), :]
                        pieces.append(piece.astype(F32))
                    lines = jnp.concatenate(pieces, axis=1)
                    lines = pltpu.roll(jnp.concatenate([lines, jnp.zeros((SUB, size), F32)], axis=0), drop, 0)
                    lines = jnp.concatenate([lines, jnp.zeros((block + SUB, width - size), F32)], axis=1)
                    turned = pltpu.roll(lines, col, 1)
                    where = pl.ds(pl.multiple_of(base + at, SUB), block + SUB)
                    total[part, where, :] = total[part, where, :] + turned
                return inner

            lax.fori_loop(0, size // block, rows, 0)
        for x in range(nx):
            for y in range(ny):
                index = x * ny + y
                first = MARGIN + index * own
                second = index * edge + (nx * ny * own if 2 * index >= nx * ny else 0)
                for side in range(2):
                    major, minor = (x, y) if side == 0 else (y, x)
                    lanes = slice(side * width // 2, (side + 1) * width // 2)
                    place = slice(3 * minor, 3 * minor + 3)
                    out[slot, side, major, place, 0:own, :] = total[:, first : first + own, lanes].astype(BF)
                    out[slot, side, major, place, own:each, :] = total[:, second : second + edge, lanes].astype(BF)
        return carry

    lax.fori_loop(0, active_slots(lax.axis_index("cuts"), lax.axis_size("cuts")), one_slot, 0)


def reduce_kernel(
    grids, owned, out,
    held, pre_up, pre_down, staged_up, staged_down, got_up, got_down, partial,
    pre_up2, pre_down2, staged_up2, staged_down2, got_up2, got_down2,
    final, extra, rows_here, ratio, incoming,
    send_sem, recv_sem, send_m, recv_m, send_d, recv_d, local_sem, held_sem,
):
    tile = lax.axis_index("tile")
    where = {"probe_0": lax.axis_index("probe_0"), "probe_1": lax.axis_index("probe_1")}
    sizes = {"probe_0": lax.axis_size("probe_0"), "probe_1": lax.axis_size("probe_1")}
    nx, ny = sizes["probe_0"], sizes["probe_1"]
    count = nx * ny
    me = where["probe_0"] * ny + where["probe_1"]
    cut = lax.axis_index("cuts")
    cuts = lax.axis_size("cuts")
    last = cuts - 3
    slots = active_slots(cut, cuts)
    each = grids.shape[4]
    own = 2 * each // 3
    edge = each - own
    lanes = grids.shape[5]
    half = count // 2
    order = (("probe_0", "probe_1"), ("probe_1", "probe_0"))

    def device(index):
        return {"tile": 1 - tile, "probe_0": index // ny, "probe_1": lax.rem(index, ny)}

    lower = me // half
    target = (1 - lower) * (count - half // 2 + me // 2) + lower * ((me - half) // 2)
    outer = where["probe_0"] // (nx - 1) + (nx - 1 - where["probe_0"]) // (nx - 1)
    source = where["probe_0"] // (nx - 1) * (2 * (me - count + half // 2)) + (
        nx - 1 - where["probe_0"]
    ) // (nx - 1) * (half + 2 * me)

    fetch = pltpu.make_async_copy(owned.at[:, pl.ds(pl.multiple_of(me * own, own), own), :], rows_here, local_sem)
    fetch.start()

    def load(slot):
        return pltpu.make_async_copy(grids.at[slot], held.at[slot], held_sem.at[slot])

    def start_load(slot, carry):
        load(slot).start()
        return carry

    lax.fori_loop(0, slots, start_load, 0)

    barrier = pltpu.get_barrier_semaphore()

    @pl.when(cut >= last)
    def _():
        host = last - 1 + cut // (last + 1)
        pl.semaphore_signal(barrier, inc=1, device_id={"cuts": host}, device_id_type=MESH_ID)

    @pl.when(cut <= last)
    def _():
        for axis in ("probe_0", "probe_1"):
            for step in (1, sizes[axis] - 1):
                other = {axis: lax.rem(where[axis] + step, sizes[axis])}
                pl.semaphore_signal(barrier, inc=1, device_id=other, device_id_type=MESH_ID)

        @pl.when(outer == 1)
        def _():
            for which in range(2):
                pl.semaphore_signal(barrier, inc=1, device_id=device(source + which), device_id_type=MESH_ID)

        pl.semaphore_wait(barrier, 5 + cut // (last - 1) + cut // last)

    def copies(slot, stage, side, src, bufs):
        axis = order[side][stage]
        size = sizes[axis]
        here = where[axis]
        plus, minus = lax.rem(here + 1, size), lax.rem(here + size - 1, size)
        opposite = lax.rem(here + 2, size)
        up_pre, down_pre, up_staged, down_staged, up_got, down_got = bufs
        depth = src.shape[1]
        cut = (depth + 1) // 2
        low, high = pl.ds(0, cut), pl.ds(cut, depth - cut)

        def copy(index, source_ref, target_ref, to):
            return pltpu.make_async_remote_copy(
                src_ref=source_ref,
                dst_ref=target_ref,
                send_sem=send_sem.at[slot, stage, side, index],
                recv_sem=recv_sem.at[slot, stage, side, index],
                device_id={axis: to},
                device_id_type=MESH_ID,
            )

        return (
            copy(0, src.at[opposite, low], up_pre.at[side], plus),
            copy(1, src.at[opposite, high], down_pre.at[side], minus),
            copy(2, src.at[plus, high], up_got.at[side, high], plus),
            copy(3, src.at[minus, low], down_got.at[side, low], minus),
            copy(4, up_staged.at[side], up_got.at[side, low], plus),
            copy(5, down_staged.at[side], down_got.at[side, high], minus),
        ), (here, plus, minus, low, high)

    def begin(slot, stage, side, src, bufs):
        made, _ = copies(slot, stage, side, src, bufs)
        for index in range(4):
            made[index].start()

    def relay(slot, stage, side, src, bufs):
        made, (_, plus, minus, low, high) = copies(slot, stage, side, src, bufs)
        up_pre, down_pre, up_staged, down_staged, _, _ = bufs
        made[0].wait_recv()
        up_staged[side] = (up_pre[side].astype(F32) + src[plus, low].astype(F32)).astype(BF)
        made[4].start()
        made[1].wait_recv()
        down_staged[side] = (down_pre[side].astype(F32) + src[minus, high].astype(F32)).astype(BF)
        made[5].start()

    def settle(slot, stage, side, src, bufs):
        made, (here, _, _, _, _) = copies(slot, stage, side, src, bufs)
        for index in range(2, 6):
            made[index].wait_recv()
        up_got, down_got = bufs[4], bufs[5]
        return src[here].astype(F32) + up_got[side].astype(F32) + down_got[side].astype(F32)

    def drain(slot, stage, side, src, bufs):
        for copy in copies(slot, stage, side, src, bufs)[0]:
            copy.wait_send()

    def ring_of(slot, buffers):
        return tuple(buffer.at[slot] for buffer in buffers)

    def margin_copy(slot, piece):
        return pltpu.make_async_remote_copy(
            src_ref=final.at[slot, :, :, pl.ds(own, edge), :],
            dst_ref=extra.at[slot, piece],
            send_sem=send_m.at[slot],
            recv_sem=recv_m.at[slot, piece],
            device_id=device(target),
            device_id_type=MESH_ID,
        )

    def deliver(slot):
        return pltpu.make_async_remote_copy(
            src_ref=ratio.at[slot],
            dst_ref=incoming,
            send_sem=send_d.at[slot],
            recv_sem=recv_d,
            device_id={"cuts": lax.rem(cut + 1 + slot * (cut - last + 1), cuts)},
            device_id_type=MESH_ID,
        )

    def one_slot(slot, carry):
        load(slot).wait()
        grid = held.at[slot]
        part_sums = partial.at[slot]
        one = ring_of(slot, (pre_up, pre_down, staged_up, staged_down, got_up, got_down))
        two = ring_of(slot, (pre_up2, pre_down2, staged_up2, staged_down2, got_up2, got_down2))
        for side in range(2):
            begin(slot, 0, side, grid.at[side], one)
        for side in range(2):
            relay(slot, 0, side, grid.at[side], one)
        for side in range(2):
            summed = settle(slot, 0, side, grid.at[side], one).astype(BF)
            for index in range(ny):
                part_sums[side, index] = summed[3 * index : 3 * index + 3]
            begin(slot, 1, side, part_sums.at[side], two)
        for side in range(2):
            relay(slot, 1, side, part_sums.at[side], two)
        for side in range(2):
            final[slot, side] = settle(slot, 1, side, part_sums.at[side], two).astype(BF)
        margin_copy(slot, lax.rem(me, 2)).start()

        @pl.when(outer == 0)
        def _():
            extra[slot] = jnp.zeros(extra.shape[1:], extra.dtype)

        @pl.when(outer == 1)
        def _():
            for piece in range(2):
                margin_copy(slot, piece).wait_recv()

        for side in range(2):
            columns = slice(side * lanes, (side + 1) * lanes)
            for piece in range(2):
                lines = slice(piece * edge, (piece + 1) * edge)
                full = final[slot, side, :, lines, :].astype(F32) + extra[slot, piece, side].astype(F32)
                scale = 1.0 / (full[2] + 1.0)
                for part in range(2):
                    ratio[slot, part, lines, columns] = full[part] * scale

        @pl.when((cut == last) | (slot > 0))
        def _():
            deliver(slot).start()

        return carry

    lax.fori_loop(0, slots, one_slot, 0)
    fetch.wait()

    @pl.when(cut < last)
    def _():
        out[...] = rows_here[...] - ratio[0]

    @pl.when(cut >= last)
    def _():
        deliver(0).wait_recv()
        out[...] = rows_here[...] - incoming[...]

    def finish(slot, carry):
        one = ring_of(slot, (pre_up, pre_down, staged_up, staged_down, got_up, got_down))
        two = ring_of(slot, (pre_up2, pre_down2, staged_up2, staged_down2, got_up2, got_down2))
        for side in range(2):
            drain(slot, 0, side, held.at[slot].at[side], one)
            drain(slot, 1, side, partial.at[slot].at[side], two)
        margin_copy(slot, lax.rem(me, 2)).wait_send()

        @pl.when((cut == last) | (slot > 0))
        def _():
            deliver(slot).wait_send()

        return carry

    lax.fori_loop(0, slots, finish, 0)


def chain_kernel(
    probe, windows, fresnel_cols, forward_rows, measured,
    grads, lights,
    cuts, forward_cols, adjoint_cols, adjoint_rows,
    waves, cots, wave_out, cot_out, total, middle, backs,
    send_f, recv_f, send_b, recv_b, send_w, recv_w,
):
    me = lax.axis_index("cuts")
    count = lax.axis_size("cuts")
    last = count - 3
    right = lax.rem(me + 1, count)
    left = lax.rem(me + count - 1, count)
    positions, chunks, size, pair = windows.shape
    half = pair // 2
    hosted = 1 + me // (last - 1)

    barrier = pltpu.get_barrier_semaphore()
    for other in (left, right):
        pl.semaphore_signal(barrier, inc=1, device_id={"cuts": other}, device_id_type=MESH_ID)

    @pl.when(me == last)
    def _():
        pl.semaphore_signal(barrier, inc=1, device_id={"cuts": count - 1}, device_id_type=MESH_ID)

    first_half, second_half = slice(0, half), slice(half, pair)

    @pl.when(me == 0)
    def _():
        for position in range(positions):
            for chunk in range(chunks):
                lanes = slice(chunk * half, (chunk + 1) * half)
                waves[0, position, chunk, :, first_half] = probe[0, :, lanes]
                waves[0, position, chunk, :, second_half] = probe[1, :, lanes]

    pl.semaphore_wait(barrier, 2 + me // (count - 1))

    def window_copy(position, slot, target):
        return pltpu.make_async_remote_copy(
            src_ref=windows.at[position],
            dst_ref=cuts.at[slot, position],
            send_sem=send_w.at[position],
            recv_sem=recv_w.at[slot, position],
            device_id={"cuts": target},
            device_id_type=MESH_ID,
        )

    give_slot = 1 - lax.rem(me + 1, 2) * (me // (last + 1))
    give_to = last - 1 + me // (last + 1)

    @pl.when(me >= last)
    def _():
        for position in range(positions):
            window_copy(position, give_slot, give_to).start()

    @pl.when(me < last)
    def _():
        cuts[0] = windows[...]

    def turned(value):
        return value.astype(F32).T.astype(BF)

    def prepare_forward(chunk, carry):
        lanes = pl.ds(pl.multiple_of(chunk * half, half), half)
        for other in range(chunks):
            lines = slice(other * half, (other + 1) * half)
            real, imag = turned(fresnel_cols[0, lines, lanes]), turned(fresnel_cols[1, lines, lanes])
            left_lanes = slice(other * pair, other * pair + half)
            right_lanes = slice(other * pair + half, (other + 1) * pair)
            forward_cols[chunk, first_half, left_lanes] = real
            forward_cols[chunk, first_half, right_lanes] = imag
            forward_cols[chunk, second_half, left_lanes] = -imag
            forward_cols[chunk, second_half, right_lanes] = real
        return carry

    def prepare_adjoint(chunk, carry):
        lines = pl.ds(pl.multiple_of(chunk * half, half), half)
        for other in range(chunks):
            lanes = slice(other * half, (other + 1) * half)
            real, imag = fresnel_cols[0, lines, lanes], fresnel_cols[1, lines, lanes]
            left_lanes = slice(other * pair, other * pair + half)
            right_lanes = slice(other * pair + half, (other + 1) * pair)
            adjoint_cols[chunk, first_half, left_lanes] = real
            adjoint_cols[chunk, first_half, right_lanes] = -imag
            adjoint_cols[chunk, second_half, left_lanes] = imag
            adjoint_cols[chunk, second_half, right_lanes] = real
            for part in range(2):
                block = forward_rows[pl.ds(pl.multiple_of(part * size + chunk * half, half), half), lanes]
                adjoint_rows[part * size + other * half : part * size + (other + 1) * half, lines] = turned(block)
        return carry

    def forward_copy(position, chunk):
        return pltpu.make_async_remote_copy(
            src_ref=wave_out.at[position, chunk],
            dst_ref=waves.at[0, position, chunk],
            send_sem=send_f.at[position, chunk],
            recv_sem=recv_f.at[position, chunk],
            device_id={"cuts": right},
            device_id_type=MESH_ID,
        )

    def adjoint_copy(position, chunk):
        return pltpu.make_async_remote_copy(
            src_ref=cot_out.at[position, chunk],
            dst_ref=cots.at[position, chunk],
            send_sem=send_b.at[position, chunk],
            recv_sem=recv_b.at[position, chunk],
            device_id={"cuts": left},
            device_id_type=MESH_ID,
        )

    def parts_of(value):
        value = value.astype(F32)
        return value[:, :half], value[:, half:]

    def both(real, imag):
        return jnp.concatenate([real, imag], axis=1)

    def add_product(chunk, value, matrix):
        product = jnp.dot(value, matrix, preferred_element_type=F32)
        if chunk == 0:
            total[...] = product
        elif chunk < chunks - 1:
            total[...] += product
        else:
            product = (total[...] + product).astype(BF)
            for other in range(chunks):
                middle[other] = product[:, other * pair : (other + 1) * pair]

    def forward(position):
        def hosted_slice(slot, carry):
            @pl.when((me >= last) | (slot > 0))
            def _():
                window_copy(position, slot, give_to).wait_recv()

            for chunk in range(chunks):
                @pl.when((me > 0) & (slot == 0))
                def _():
                    forward_copy(position, chunk).wait_recv()

                wave_r, wave_i = parts_of(waves[slot, position, chunk])
                win_r, win_i = parts_of(cuts[slot, position, chunk])
                out = both(wave_r * win_r - wave_i * win_i, wave_r * win_i + wave_i * win_r).astype(BF)
                add_product(chunk, out, forward_cols[chunk])

            def produce(chunk, inner):
                result = jnp.dot(forward_rows[...], middle[chunk], preferred_element_type=F32)
                real = result[:size, :half] - result[size:, half:]
                imag = result[size:, :half] + result[:size, half:]
                value = both(real, imag).astype(BF)

                @pl.when(slot < hosted - 1)
                def _():
                    waves[1, position, chunk] = value

                @pl.when(slot == hosted - 1)
                def _():
                    wave_out[position, chunk] = value

                    @pl.when(me < last)
                    def _():
                        forward_copy(position, chunk).start()

                    @pl.when(me == last)
                    def _():
                        psi_r, psi_i = parts_of(value)
                        amplitude = measured[position, :, pl.ds(pl.multiple_of(chunk * half, half), half)]
                        factor = 1.0 - amplitude * lax.rsqrt(psi_r * psi_r + psi_i * psi_i + 1.0)
                        cots[position, chunk] = both(psi_r * factor, psi_i * factor).astype(BF)

                return inner

            lax.fori_loop(0, chunks, produce, 0)

            def brighten(chunk, inner):
                wave_r, wave_i = parts_of(waves[slot, position, chunk])
                lights[slot, position, chunk] = (wave_r * wave_r + wave_i * wave_i).astype(BF)
                return inner

            lax.fori_loop(0, chunks, brighten, 0)
            return carry

        lax.fori_loop(0, hosted, hosted_slice, 0)

    def adjoint(position):
        def hosted_slice(step, carry):
            slot = hosted - 1 - step
            for chunk in range(chunks):
                @pl.when((me < last) & (step == 0))
                def _():
                    adjoint_copy(position, chunk).wait_recv()

                add_product(chunk, cots[position, chunk], adjoint_cols[chunk])

            def produce(chunk, inner):
                result = jnp.dot(adjoint_rows[...], middle[chunk], preferred_element_type=F32)
                real = result[:size, :half] + result[size:, half:]
                imag = result[:size, half:] - result[size:, :half]
                back = both(real, imag).astype(BF)
                backs[chunk] = back

                @pl.when(me > 0)
                def _():
                    back_r, back_i = parts_of(back)
                    win_r, win_i = parts_of(cuts[slot, position, chunk])
                    value = both(win_r * back_r + win_i * back_i, win_r * back_i - win_i * back_r).astype(BF)

                    @pl.when(slot > 0)
                    def _():
                        cots[position, chunk] = value

                    @pl.when(slot == 0)
                    def _():
                        cot_out[position, chunk] = value
                        adjoint_copy(position, chunk).start()

                return inner

            lax.fori_loop(0, chunks, produce, 0)

            def grade(chunk, inner):
                wave_r, wave_i = parts_of(waves[slot, position, chunk])
                back_r, back_i = parts_of(backs[chunk])
                grads[slot, position, chunk] = both(
                    wave_r * back_r + wave_i * back_i, wave_r * back_i - wave_i * back_r
                ).astype(BF)
                return inner

            lax.fori_loop(0, chunks, grade, 0)
            return carry

        lax.fori_loop(0, hosted, hosted_slice, 0)

    late = me // last

    @pl.when(me <= last)
    def _():
        lax.fori_loop(0, chunks, prepare_forward, 0)

        def phase(step, carry):
            is_back = late * (step % positions) + (1 - late) * (step // positions)
            position = late * (step // positions) + (1 - late) * (step % positions)

            @pl.when(step == positions * (1 - late))
            def _():
                lax.fori_loop(0, chunks, prepare_adjoint, 0)

            @pl.when(is_back == 0)
            def _():
                forward(position)

            @pl.when(is_back == 1)
            def _():
                adjoint(position)

            return carry

        lax.fori_loop(0, 2 * positions, phase, 0)

    def finish(index, carry):
        position = index // chunks
        chunk = index % chunks

        @pl.when(me < last)
        def _():
            forward_copy(position, chunk).wait_send()

        @pl.when((me > 0) & (me <= last))
        def _():
            adjoint_copy(position, chunk).wait_send()

        return carry

    lax.fori_loop(0, positions * chunks, finish, 0)

    @pl.when(me >= last)
    def _():
        for position in range(positions):
            window_copy(position, give_slot, give_to).wait_send()


def in_vmem(count):
    return [pl.BlockSpec(memory_space=pltpu.VMEM)] * count


def in_smem():
    return [pl.BlockSpec(memory_space=pltpu.SMEM)]


def on_chip(limit, **more):
    return pltpu.CompilerParams(vmem_limit_bytes=limit * 2**20, **more)


def run_chain(probe_wave, windows, fresnel_cols, fresnel_rows, amplitude):
    positions, chunks, size, pair = windows.shape
    dma = pltpu.SemaphoreType.DMA
    wave_stack = VMEM((positions, chunks, size, pair), BF)
    hosted_stack = VMEM((HOSTED, positions, chunks, size, pair), BF)
    columns = VMEM((chunks, pair, 2 * size), BF)
    return pl.pallas_call(
        chain_kernel,
        out_shape=[
            jax.ShapeDtypeStruct((HOSTED, positions, chunks, size, pair), BF),
            jax.ShapeDtypeStruct((HOSTED, positions, chunks, size, LANES), BF),
        ],
        in_specs=in_vmem(5),
        out_specs=in_vmem(2),
        scratch_shapes=[
            hosted_stack,
            columns,
            columns,
            VMEM((2 * size, size), BF),
            hosted_stack,
            wave_stack,
            wave_stack,
            wave_stack,
            VMEM((size, 2 * size), F32),
            VMEM((chunks, size, pair), BF),
            VMEM((chunks, size, pair), BF),
            dma((positions, chunks)),
            dma((positions, chunks)),
            dma((positions, chunks)),
            dma((positions, chunks)),
            dma((positions,)),
            dma((HOSTED, positions)),
        ],
        compiler_params=on_chip(60, collective_id=0, has_side_effects=True),
        name="chain",
    )(probe_wave, windows, fresnel_cols, fresnel_rows.reshape(2 * size, size), amplitude)


def shards(probe_wave, fresnel_rows, fresnel_cols, object_slices, offsets, measured):
    owned = object_slices[0]
    starts = offsets[0]
    size = probe_wave.shape[1]
    positions = starts.shape[0]
    rows, width = owned.shape[1:]
    chunks = size // LANES
    pair = 2 * LANES
    nx, ny = lax.axis_size("probe_0"), lax.axis_size("probe_1")
    count = nx * ny
    share = 2 * MARGIN // count
    own = rows // count
    each = own + share
    dma = pltpu.SemaphoreType.DMA

    edges = pl.pallas_call(
        edge_kernel,
        out_shape=jax.ShapeDtypeStruct((count, 2, share, width), BF),
        in_specs=in_vmem(1),
        out_specs=pl.BlockSpec(memory_space=pltpu.VMEM),
        scratch_shapes=[
            VMEM((2, share, width), BF),
            VMEM((2, share, width), BF),
            VMEM((count, 2, share, width), BF),
            dma,
            dma,
            dma((count,)),
            dma((count,)),
        ],
        compiler_params=on_chip(24, collective_id=1, has_side_effects=True),
        name="edge",
    )(owned)

    windows = pl.pallas_call(
        cut_kernel,
        out_shape=jax.ShapeDtypeStruct((positions, chunks, size, pair), BF),
        in_specs=in_smem() + in_vmem(2),
        out_specs=pl.BlockSpec(memory_space=pltpu.VMEM),
        scratch_shapes=[VMEM((2, rows + 2 * MARGIN + SUB, width), F32)],
        compiler_params=on_chip(40),
        name="cut",
    )(starts, owned, edges)

    grads, lights = run_chain(probe_wave, windows, fresnel_cols, fresnel_rows, measured[0])

    grid = pl.pallas_call(
        place_kernel,
        out_shape=jax.ShapeDtypeStruct((HOSTED, 2, nx, 3 * ny, each, width // 2), BF),
        in_specs=in_smem() + in_vmem(2),
        out_specs=pl.BlockSpec(memory_space=pltpu.VMEM),
        scratch_shapes=[VMEM((3, rows + 2 * MARGIN + SUB, width), F32)],
        compiler_params=on_chip(48),
        name="place",
    )(starts, grads, lights)

    def slots(depth):
        return VMEM((HOSTED, 2, depth, each, width // 2), BF)

    def ring(depth):
        cut = (depth + 1) // 2
        return [slots(cut), slots(depth - cut), slots(cut), slots(depth - cut), slots(depth), slots(depth)]

    updated = pl.pallas_call(
        reduce_kernel,
        out_shape=jax.ShapeDtypeStruct((2, own, width), F32),
        in_specs=[pl.BlockSpec(memory_space=pl.ANY)] * 2,
        out_specs=pl.BlockSpec(memory_space=pltpu.VMEM),
        scratch_shapes=[VMEM((HOSTED, 2, nx, 3 * ny, each, width // 2), BF)]
        + ring(3 * ny)
        + [VMEM((HOSTED, 2, ny, 3, each, width // 2), BF)]
        + ring(3)
        + [
            slots(3),
            VMEM((HOSTED, 2, 2, 3, share, width // 2), BF),
            VMEM((2, own, width), F32),
            VMEM((HOSTED, 2, own, width), F32),
            VMEM((2, own, width), F32),
            dma((HOSTED, 2, 2, 6)),
            dma((HOSTED, 2, 2, 6)),
            dma((HOSTED,)),
            dma((HOSTED, 2)),
            dma((HOSTED,)),
            dma,
            dma,
            dma((HOSTED,)),
        ],
        compiler_params=on_chip(56, collective_id=2, has_side_effects=True),
        name="reduce",
    )(grid, owned)
    return updated[None]


def solution(mesh):
    split = Mesh(
        mesh.devices.reshape(mesh.shape["cuts"], mesh.shape["tile"], 4, 4),
        ("cuts", "tile", "probe_0", "probe_1"),
    )
    return jax.shard_map(
        shards,
        mesh=split,
        in_specs=(
            P(),
            P(),
            P(),
            P("cuts", None, "tile", None),
            P("tile", PROBE, None),
            P("tile", PROBE, None, None),
        ),
        out_specs=P("cuts", None, TILE_PROBE, None),
        check_vma=False,
    )
```

```python
import jax
import jax.numpy as jnp
from jax import lax
from jax.experimental import pallas as pl
from jax.experimental.pallas import tpu as pltpu
from jax.sharding import Mesh
from jax.sharding import PartitionSpec as P

MARGIN = 128
LANES = 128
HOSTED = 2
LIGHT, GRADE = 0, 1
PROBE = ("probe_0", "probe_1")
TILE_PROBE = ("tile", "probe_0", "probe_1")
MESH_ID = pl.DeviceIdType.MESH
BF = jnp.bfloat16
F32 = jnp.float32
VMEM = pltpu.VMEM


def active_slots(me, count):
    return (1 + me // (count - 4)) * (1 - me // (count - 2))


def step_kernel(
    starts, owned, probe, fresnel_cols, forward_rows, measured,
    out,
    rows_here, edge_rows, mine, swapped, gathered, slab, tall, wide, amplitude_here,
    cuts, forward_cols, adjoint_cols, adjoint_rows,
    waves, cots, wave_out, cot_out, total, middle, backs,
    pieces, grids, pre, staged, got_up, got_down, partial, pre2, staged2, got_up2, got_down2,
    final, extra, ratio, incoming,
    send_z, recv_z, send_e, recv_e,
    send_f, recv_f, send_b, recv_b, send_w, recv_w,
    send_r, recv_r, send_m, recv_m, send_d, recv_d, local_sem,
):
    tile = lax.axis_index("tile")
    where = {"probe_0": lax.axis_index("probe_0"), "probe_1": lax.axis_index("probe_1")}
    sizes = {"probe_0": lax.axis_size("probe_0"), "probe_1": lax.axis_size("probe_1")}
    nx, ny = sizes["probe_0"], sizes["probe_1"]
    members = nx * ny
    spot = where["probe_0"] * ny + where["probe_1"]
    me = lax.axis_index("cuts")
    count = lax.axis_size("cuts")
    last = count - 3
    right = lax.rem(me + 1, count)
    left = lax.rem(me + count - 1, count)
    _, positions, chunks, size, pair = cuts.shape
    half = pair // 2
    hosted = 1 + me // (last - 1)
    slots = active_slots(me, count)
    _, rows, width = owned.shape
    share = mine.shape[1]
    own = rows // members
    each = own + share
    lanes_side = width // 2

    def plane_peer(step):
        other = lax.rem(spot + step, members)
        return {"probe_0": other // ny, "probe_1": lax.rem(other, ny)}

    def across(index):
        return {"tile": 1 - tile, "probe_0": index // ny, "probe_1": lax.rem(index, ny)}

    lower = spot // (members // 2)
    edge_first = (1 - lower) * (rows - MARGIN + spot * share) + lower * (spot - members // 2) * share
    target = (1 - lower) * (members - members // 4 + spot // 2) + lower * ((spot - members // 2) // 2)
    at_end = where["probe_0"] // (nx - 1)
    at_start = (nx - 1 - where["probe_0"]) // (nx - 1)
    outer = at_end + at_start
    source = at_end * (2 * (spot - members + members // 4)) + at_start * (members // 2 + 2 * spot)

    barrier = pltpu.get_barrier_semaphore()

    def greet(device_id):
        pl.semaphore_signal(barrier, inc=1, device_id=device_id, device_id_type=MESH_ID)

    greet({"tile": 1 - tile})
    for step in range(1, members):
        greet(plane_peer(step))
    for other in (left, right):
        greet({"cuts": other})

    @pl.when(me == last)
    def _():
        greet({"cuts": count - 1})

    @pl.when(me == count - 1)
    def _():
        greet({"cuts": last})

    @pl.when(outer == 1)
    def _():
        for which in range(2):
            greet(across(source + which))

    fetch_edge = pltpu.make_async_copy(
        owned.at[:, pl.ds(pl.multiple_of(edge_first, share), share), :], edge_rows, local_sem.at[0]
    )
    fetch_edge.start()
    fetch_rows = pltpu.make_async_copy(
        owned.at[:, pl.ds(pl.multiple_of(spot * own, own), own), :], rows_here, local_sem.at[1]
    )
    fetch_rows.start()

    def fetch_slab(part):
        return pltpu.make_async_copy(owned.at[part], total.at[:, pl.ds(0, width)], local_sem.at[2])

    fetch_slab(0).start()

    def fetch_measured():
        return pltpu.make_async_copy(measured, amplitude_here, local_sem.at[3])

    @pl.when(me == last)
    def _():
        fetch_measured().start()

    fetch_edge.wait()
    mine[...] = edge_rows[...].astype(BF)
    pl.semaphore_wait(barrier, members + 3 + (me + 1) // count + (me // last) * (1 - me // (last + 1)))

    swap = pltpu.make_async_remote_copy(
        src_ref=mine, dst_ref=swapped, send_sem=send_z, recv_sem=recv_z, device_id={"tile": 1 - tile}, device_id_type=MESH_ID
    )
    swap.start()

    first_half, second_half = slice(0, half), slice(half, pair)

    @pl.when(me == 0)
    def _():
        for position in range(positions):
            for chunk in range(chunks):
                lanes = slice(chunk * half, (chunk + 1) * half)
                waves[0, position, chunk, :, first_half] = probe[0, :, lanes]
                waves[0, position, chunk, :, second_half] = probe[1, :, lanes]

    def turned(value):
        return value.astype(F32).T.astype(BF)

    def prepare_forward(chunk, carry):
        lanes = pl.ds(pl.multiple_of(chunk * half, half), half)
        for other in range(chunks):
            lines = slice(other * half, (other + 1) * half)
            real, imag = turned(fresnel_cols[0, lines, lanes]), turned(fresnel_cols[1, lines, lanes])
            left_lanes = slice(other * pair, other * pair + half)
            right_lanes = slice(other * pair + half, (other + 1) * pair)
            forward_cols[chunk, first_half, left_lanes] = real
            forward_cols[chunk, first_half, right_lanes] = imag
            forward_cols[chunk, second_half, left_lanes] = -imag
            forward_cols[chunk, second_half, right_lanes] = real
        return carry

    def prepare_adjoint(chunk, carry):
        lines = pl.ds(pl.multiple_of(chunk * half, half), half)
        for other in range(chunks):
            lanes = slice(other * half, (other + 1) * half)
            real, imag = fresnel_cols[0, lines, lanes], fresnel_cols[1, lines, lanes]
            left_lanes = slice(other * pair, other * pair + half)
            right_lanes = slice(other * pair + half, (other + 1) * pair)
            adjoint_cols[chunk, first_half, left_lanes] = real
            adjoint_cols[chunk, first_half, right_lanes] = -imag
            adjoint_cols[chunk, second_half, left_lanes] = imag
            adjoint_cols[chunk, second_half, right_lanes] = real
            for part in range(2):
                block = forward_rows[pl.ds(pl.multiple_of(part * size + chunk * half, half), half), lanes]
                adjoint_rows[part * size + other * half : part * size + (other + 1) * half, lines] = turned(block)
        return carry


    for part in range(2):
        fetch_slab(part).wait()
        slab[part, MARGIN : MARGIN + rows, :] = total[:, :width].astype(BF)
        if part == 0:
            fetch_slab(1).start()

    def edge_copy(step, slot):
        return pltpu.make_async_remote_copy(
            src_ref=swapped,
            dst_ref=gathered.at[slot],
            send_sem=send_e.at[step],
            recv_sem=recv_e.at[slot],
            device_id=plane_peer(step),
            device_id_type=MESH_ID,
        )

    swap.wait_recv()
    for step in range(1, members):
        edge_copy(step, spot).start()
    gathered[spot] = swapped[...]

    lax.fori_loop(0, chunks, prepare_forward, 0)
    lax.fori_loop(0, chunks, prepare_adjoint, 0)

    def select(index, carry):
        position, which = index // 2, lax.rem(index, 2)
        start = starts[position, which]
        far = lax.broadcasted_iota(jnp.int32, (width, size), 0) - lax.broadcasted_iota(jnp.int32, (width, size), 1)
        tall[position, which] = jnp.where(far == start, 1.0, 0.0).astype(BF)
        far = lax.broadcasted_iota(jnp.int32, (size, width), 1) - lax.broadcasted_iota(jnp.int32, (size, width), 0)
        wide[position, which] = jnp.where(far == start, 1.0, 0.0).astype(BF)
        return carry

    lax.fori_loop(0, 2 * positions, select, 0)

    for step in range(1, members):
        edge_copy(step, lax.rem(spot + members - step, members)).wait_recv()
    for index in range(members):
        first = index * share + (rows if index >= members // 2 else 0)
        slab[:, first : first + share, :] = gathered[index]

    def cut_window(position):
        def columns(index, carry):
            part, where_to = index // 2, lax.rem(index, 2)
            lanes = pl.ds(pl.multiple_of(where_to * pair, pair), pair)
            values = jnp.dot(slab[part], tall[position, 1, :, lanes], preferred_element_type=F32).astype(BF)
            values = jnp.dot(wide[position, 0], values, preferred_element_type=F32).astype(BF)
            here = pl.ds(pl.multiple_of(part * half, half), half)
            wave_out[position, 2 * where_to, :, here] = values[:, :half]
            wave_out[position, 2 * where_to + 1, :, here] = values[:, half:]
            return carry

        lax.fori_loop(0, 4, columns, 0)

    def window_copy(position, slot, to):
        return pltpu.make_async_remote_copy(
            src_ref=wave_out.at[position],
            dst_ref=cuts.at[slot, position],
            send_sem=send_w.at[position],
            recv_sem=recv_w.at[slot, position],
            device_id={"cuts": to},
            device_id_type=MESH_ID,
        )

    give_slot = 1 - lax.rem(me + 1, 2) * (me // (last + 1))
    give_to = last - 1 + me // (last + 1)

    @pl.when(me >= last)
    def _():
        for position in range(positions):
            cut_window(position)
            window_copy(position, give_slot, give_to).start()

    @pl.when(me == last)
    def _():
        fetch_measured().wait()

    def forward_copy(position, chunk):
        return pltpu.make_async_remote_copy(
            src_ref=wave_out.at[position, chunk],
            dst_ref=waves.at[0, position, chunk],
            send_sem=send_f.at[position, chunk],
            recv_sem=recv_f.at[position, chunk],
            device_id={"cuts": right},
            device_id_type=MESH_ID,
        )

    def adjoint_copy(position, chunk):
        return pltpu.make_async_remote_copy(
            src_ref=cot_out.at[position, chunk],
            dst_ref=cots.at[position, chunk],
            send_sem=send_b.at[position, chunk],
            recv_sem=recv_b.at[position, chunk],
            device_id={"cuts": left},
            device_id_type=MESH_ID,
        )

    def parts_of(value):
        value = value.astype(F32)
        return value[:, :half], value[:, half:]

    def both(real, imag):
        return jnp.concatenate([real, imag], axis=1)

    def add_product(chunk, value, matrix):
        product = jnp.dot(value, matrix, preferred_element_type=F32)
        if chunk == 0:
            total[...] = product
        elif chunk < chunks - 1:
            total[...] += product
        else:
            product = (total[...] + product).astype(BF)
            for other in range(chunks):
                middle[other] = product[:, other * pair : (other + 1) * pair]

    def forward(position):
        @pl.when(me < last)
        def _():
            cut_window(position)
            cuts[0, position] = wave_out[position]

        def hosted_slice(slot, carry):
            @pl.when((me >= last) | (slot > 0))
            def _():
                window_copy(position, slot, give_to).wait_recv()

            for chunk in range(chunks):
                @pl.when((me > 0) & (slot == 0))
                def _():
                    forward_copy(position, chunk).wait_recv()

                wave_r, wave_i = parts_of(waves[slot, position, chunk])
                win_r, win_i = parts_of(cuts[slot, position, chunk])
                out = both(wave_r * win_r - wave_i * win_i, wave_r * win_i + wave_i * win_r).astype(BF)
                add_product(chunk, out, forward_cols[chunk])

            def produce(chunk, inner):
                result = jnp.dot(forward_rows[...], middle[chunk], preferred_element_type=F32)
                real = result[:size, :half] - result[size:, half:]
                imag = result[size:, :half] + result[:size, half:]
                value = both(real, imag).astype(BF)

                @pl.when(slot < hosted - 1)
                def _():
                    waves[1, position, chunk] = value

                @pl.when(slot == hosted - 1)
                def _():
                    @pl.when(me < last)
                    def _():
                        wave_out[position, chunk] = value
                        forward_copy(position, chunk).start()

                    @pl.when(me == last)
                    def _():
                        psi_r, psi_i = parts_of(value)
                        amplitude = amplitude_here[position, :, pl.ds(pl.multiple_of(chunk * half, half), half)]
                        factor = 1.0 - amplitude * lax.rsqrt(psi_r * psi_r + psi_i * psi_i + 1.0)
                        cots[position, chunk] = both(psi_r * factor, psi_i * factor).astype(BF)

                return inner

            lax.fori_loop(0, chunks, produce, 0)

            def brighten(chunk, inner):
                wave_r, wave_i = parts_of(waves[slot, position, chunk])
                lanes = pl.ds(pl.multiple_of(chunk * half, half), half)
                pieces[slot, position, 2, :, lanes] = (wave_r * wave_r + wave_i * wave_i).astype(BF)
                return inner

            lax.fori_loop(0, chunks, brighten, 0)
            return carry

        lax.fori_loop(0, hosted, hosted_slice, 0)

    def adjoint(position):
        def hosted_slice(step, carry):
            slot = hosted - 1 - step
            for chunk in range(chunks):
                @pl.when((me < last) & (step == 0))
                def _():
                    adjoint_copy(position, chunk).wait_recv()

                add_product(chunk, cots[position, chunk], adjoint_cols[chunk])

            def produce(chunk, inner):
                result = jnp.dot(adjoint_rows[...], middle[chunk], preferred_element_type=F32)
                real = result[:size, :half] + result[size:, half:]
                imag = result[:size, half:] - result[size:, :half]
                back = both(real, imag).astype(BF)
                backs[chunk] = back

                @pl.when(me > 0)
                def _():
                    back_r, back_i = parts_of(back)
                    win_r, win_i = parts_of(cuts[slot, position, chunk])
                    value = both(win_r * back_r + win_i * back_i, win_r * back_i - win_i * back_r).astype(BF)

                    @pl.when(slot > 0)
                    def _():
                        cots[position, chunk] = value

                    @pl.when(slot == 0)
                    def _():
                        cot_out[position, chunk] = value
                        adjoint_copy(position, chunk).start()

                return inner

            lax.fori_loop(0, chunks, produce, 0)

            def grade(chunk, inner):
                wave_r, wave_i = parts_of(waves[slot, position, chunk])
                back_r, back_i = parts_of(backs[chunk])
                lanes = pl.ds(pl.multiple_of(chunk * half, half), half)
                pieces[slot, position, 0, :, lanes] = (wave_r * back_r + wave_i * back_i).astype(BF)
                pieces[slot, position, 1, :, lanes] = (wave_r * back_i - wave_i * back_r).astype(BF)
                return inner

            lax.fori_loop(0, chunks, grade, 0)
            return carry

        lax.fori_loop(0, hosted, hosted_slice, 0)


    def place(slot, part, position):
        for side in range(2):
            lanes = slice(side * lanes_side, (side + 1) * lanes_side)
            values = jnp.dot(pieces[slot, position, part], wide[position, 1, :, lanes], preferred_element_type=F32)
            values = jnp.dot(tall[position, 0], values.astype(BF), preferred_element_type=F32)

            def put(add):
                for x in range(nx):
                    for y in range(ny):
                        index = x * ny + y
                        major, minor = (x, y) if side == 0 else (y, x)
                        first = MARGIN + index * own
                        second = index * share + (rows if 2 * index >= members else 0)
                        for at, depth, begins in ((0, own, first), (own, share, second)):
                            there = (slot, side, major, part * ny + minor, pl.ds(at, depth))
                            piece = values[begins : begins + depth]
                            if add:
                                piece = piece + grids[there].astype(F32)
                            grids[there] = piece.astype(BF)

            @pl.when(position == 0)
            def _():
                put(False)

            @pl.when(position > 0)
            def _():
                put(True)

    order = (("probe_0", "probe_1"), ("probe_1", "probe_0"))
    parts_in = {LIGHT: (2,), GRADE: (0, 1)}

    def regions(kind, stage):
        parts = parts_in[kind]
        depth = len(parts) * (ny if stage == 0 else 1)
        first = parts[0] * (ny if stage == 0 else 1)
        if depth == 1:
            cut = each // 3 * 2
            return (pl.ds(first, 1), pl.ds(0, cut)), (pl.ds(first, 1), pl.ds(cut, each - cut))
        cut = depth // 2
        return (pl.ds(first, cut), pl.ds(0, each)), (pl.ds(first + cut, depth - cut), pl.ds(0, each))

    def buffers(slot, stage, side):
        if stage == 0:
            return grids.at[slot, side], tuple(ref.at[slot, side] for ref in (pre, staged, got_up, got_down))
        return partial.at[slot, side], tuple(ref.at[slot, side] for ref in (pre2, staged2, got_up2, got_down2))

    def ring(kind, slot, stage, side):
        axis = order[side][stage]
        length = sizes[axis]
        here = where[axis]
        plus, minus = lax.rem(here + 1, length), lax.rem(here + length - 1, length)
        opposite = lax.rem(here + 2, length)
        src, (before, queued, up, down) = buffers(slot, stage, side)
        low, high = regions(kind, stage)

        def copy(index, source_ref, target_ref, to):
            return pltpu.make_async_remote_copy(
                src_ref=source_ref,
                dst_ref=target_ref,
                send_sem=send_r.at[slot, kind, stage, side, index],
                recv_sem=recv_r.at[slot, kind, stage, side, index],
                device_id={axis: to},
                device_id_type=MESH_ID,
            )

        def make(index):
            if index == 0:
                return copy(0, src.at[(opposite, *low)], before.at[low], plus)
            if index == 1:
                return copy(1, src.at[(opposite, *high)], before.at[high], minus)
            if index == 2:
                return copy(2, src.at[(plus, *high)], up.at[high], plus)
            if index == 3:
                return copy(3, src.at[(minus, *low)], down.at[low], minus)
            if index == 4:
                return copy(4, queued.at[low], up.at[low], plus)
            return copy(5, queued.at[high], down.at[high], minus)

        return make, here, plus, minus, low, high

    def begin(kind, slot, stage, side):
        make = ring(kind, slot, stage, side)[0]
        for index in range(4):
            make(index).start()

    def relay(kind, slot, stage, side):
        make, _, plus, minus, low, high = ring(kind, slot, stage, side)
        src, (before, queued, _, _) = buffers(slot, stage, side)
        make(0).wait_recv()
        queued[low] = (before[low].astype(F32) + src[(plus, *low)].astype(F32)).astype(BF)
        make(4).start()
        make(1).wait_recv()
        queued[high] = (before[high].astype(F32) + src[(minus, *high)].astype(F32)).astype(BF)
        make(5).start()

    def settle(kind, slot, stage, side):
        make, here, _, _, _, _ = ring(kind, slot, stage, side)
        src, (_, _, up, down) = buffers(slot, stage, side)
        for index in range(2, 6):
            make(index).wait_recv()
        for part in parts_in[kind]:
            if stage == 0:
                for minor in range(ny):
                    index = part * ny + minor
                    summed = src[here, index].astype(F32) + up[index].astype(F32) + down[index].astype(F32)
                    partial[slot, side, minor, part] = summed.astype(BF)
            else:
                summed = src[here, part].astype(F32) + up[part].astype(F32) + down[part].astype(F32)
                final[slot, side, part] = summed.astype(BF)

    def drain(kind, slot, stage, side):
        make = ring(kind, slot, stage, side)[0]
        for index in range(6):
            make(index).wait_send()

    def both_sides(function, kind, stage):
        def one(slot, carry):
            for side in range(2):
                function(kind, slot, stage, side)
            return carry

        lax.fori_loop(0, slots, one, 0)

    def scatter(kinds):
        for stage in range(2):
            for function in (begin, relay, settle):
                for kind in kinds:
                    both_sides(function, kind, stage)

    early = me < last - 1
    late = me // last

    @pl.when(me <= last)
    def _():
        def phase(step, carry):
            is_back = late * (step % positions) + (1 - late) * (step // positions)
            position = late * (step // positions) + (1 - late) * (step % positions)

            @pl.when(is_back == 0)
            def _():
                forward(position)

            @pl.when(is_back == 1)
            def _():
                adjoint(position)

            @pl.when(early)
            def _():
                def one_part(index, inner):
                    place(0, 2 * (1 - is_back) + index, position)
                    return inner

                lax.fori_loop(0, 1 + is_back, one_part, 0)

            @pl.when(early & (step == positions - 1))
            def _():
                scatter((LIGHT,))

            return carry

        lax.fori_loop(0, 2 * positions, phase, 0)

        @pl.when(early)
        def _():
            scatter((GRADE,))

        @pl.when(me >= last - 1)
        def _():
            def place_one(index, carry):
                rest = lax.rem(index, 3 * positions)
                place(index // (3 * positions), lax.rem(rest, 3), rest // 3)
                return carry

            lax.fori_loop(0, slots * 3 * positions, place_one, 0)
            scatter((LIGHT, GRADE))

    def margin_copy(slot, piece):
        return pltpu.make_async_remote_copy(
            src_ref=final.at[slot, :, :, pl.ds(own, share), :],
            dst_ref=extra.at[slot, piece],
            send_sem=send_m.at[slot],
            recv_sem=recv_m.at[slot, piece],
            device_id=across(target),
            device_id_type=MESH_ID,
        )

    def deliver(slot):
        return pltpu.make_async_remote_copy(
            src_ref=ratio.at[slot],
            dst_ref=incoming,
            send_sem=send_d.at[slot],
            recv_sem=recv_d,
            device_id={"cuts": lax.rem(me + 1 + slot * (me - last + 1), count)},
            device_id_type=MESH_ID,
        )

    def start_margin(slot, carry):
        margin_copy(slot, lax.rem(spot, 2)).start()
        return carry

    lax.fori_loop(0, slots, start_margin, 0)

    def divide(slot, carry):
        @pl.when(outer == 0)
        def _():
            extra[slot] = jnp.zeros(extra.shape[1:], extra.dtype)

        @pl.when(outer == 1)
        def _():
            for piece in range(2):
                margin_copy(slot, piece).wait_recv()

        for side in range(2):
            columns = slice(side * lanes_side, (side + 1) * lanes_side)
            for piece in range(2):
                lines = slice(piece * share, (piece + 1) * share)
                full = final[slot, side, :, lines, :].astype(F32) + extra[slot, piece, side].astype(F32)
                scale = 1.0 / (full[2] + 1.0)
                for part in range(2):
                    ratio[slot, part, lines, columns] = full[part] * scale

        @pl.when((me == last) | (slot > 0))
        def _():
            deliver(slot).start()

        return carry

    lax.fori_loop(0, slots, divide, 0)
    fetch_rows.wait()

    @pl.when(me < last)
    def _():
        out[...] = rows_here[...] - ratio[0]

    @pl.when(me >= last)
    def _():
        deliver(0).wait_recv()
        out[...] = rows_here[...] - incoming[...]

    swap.wait_send()
    for step in range(1, members):
        edge_copy(step, spot).wait_send()

    def finish(index, carry):
        position = index // chunks
        chunk = index % chunks

        @pl.when(me < last)
        def _():
            forward_copy(position, chunk).wait_send()

        @pl.when((me > 0) & (me <= last))
        def _():
            adjoint_copy(position, chunk).wait_send()

        return carry

    lax.fori_loop(0, positions * chunks, finish, 0)

    @pl.when(me >= last)
    def _():
        for position in range(positions):
            window_copy(position, give_slot, give_to).wait_send()

    for kind in (LIGHT, GRADE):
        for stage in range(2):
            both_sides(drain, kind, stage)

    def finish_slot(slot, carry):
        margin_copy(slot, lax.rem(spot, 2)).wait_send()

        @pl.when((me == last) | (slot > 0))
        def _():
            deliver(slot).wait_send()

        return carry

    lax.fori_loop(0, slots, finish_slot, 0)


def shards(probe_wave, fresnel_rows, fresnel_cols, object_slices, offsets, measured):
    owned = object_slices[0]
    starts = offsets[0]
    size = probe_wave.shape[1]
    positions = starts.shape[0]
    rows, width = owned.shape[1:]
    chunks = size // LANES
    pair = 2 * LANES
    nx, ny = lax.axis_size("probe_0"), lax.axis_size("probe_1")
    count = nx * ny
    share = 2 * MARGIN // count
    own = rows // count
    each = own + share
    lanes = width // 2
    dma = pltpu.SemaphoreType.DMA
    stack = (positions, chunks, size, pair)
    block = (HOSTED, 2, 3 * ny, each, lanes)
    small = (HOSTED, 2, 3, each, lanes)
    flags = (positions, chunks)
    anywhere = pl.BlockSpec(memory_space=pl.ANY)
    vmem = pl.BlockSpec(memory_space=pltpu.VMEM)

    updated = pl.pallas_call(
        step_kernel,
        out_shape=jax.ShapeDtypeStruct((2, own, width), F32),
        in_specs=[pl.BlockSpec(memory_space=pltpu.SMEM), anywhere, vmem, vmem, vmem, anywhere],
        out_specs=vmem,
        scratch_shapes=[
            VMEM((2, own, width), F32),
            VMEM((2, share, width), F32),
            VMEM((2, share, width), BF),
            VMEM((2, share, width), BF),
            VMEM((count, 2, share, width), BF),
            VMEM((2, rows + 2 * MARGIN, width), BF),
            VMEM((positions, 2, width, size), BF),
            VMEM((positions, 2, size, width), BF),
            VMEM((positions, size, size), F32),
            VMEM((HOSTED, *stack), BF),
            VMEM((chunks, pair, 2 * size), BF),
            VMEM((chunks, pair, 2 * size), BF),
            VMEM((2 * size, size), BF),
            VMEM((HOSTED, *stack), BF),
            VMEM(stack, BF),
            VMEM(stack, BF),
            VMEM(stack, BF),
            VMEM((size, 2 * size), F32),
            VMEM((chunks, size, pair), BF),
            VMEM((chunks, size, pair), BF),
            VMEM((HOSTED, positions, 3, size, size), BF),
            VMEM((HOSTED, 2, nx, 3 * ny, each, lanes), BF),
            VMEM(block, BF),
            VMEM(block, BF),
            VMEM(block, BF),
            VMEM(block, BF),
            VMEM((HOSTED, 2, ny, 3, each, lanes), BF),
            VMEM(small, BF),
            VMEM(small, BF),
            VMEM(small, BF),
            VMEM(small, BF),
            VMEM(small, BF),
            VMEM((HOSTED, 2, 2, 3, share, lanes), BF),
            VMEM((HOSTED, 2, own, width), F32),
            VMEM((2, own, width), F32),
            dma,
            dma,
            dma((count,)),
            dma((count,)),
            dma(flags),
            dma(flags),
            dma(flags),
            dma(flags),
            dma((positions,)),
            dma((HOSTED, positions)),
            dma((HOSTED, 2, 2, 2, 6)),
            dma((HOSTED, 2, 2, 2, 6)),
            dma((HOSTED,)),
            dma((HOSTED, 2)),
            dma((HOSTED,)),
            dma,
            dma((4,)),
        ],
        compiler_params=pltpu.CompilerParams(collective_id=0, has_side_effects=True, vmem_limit_bytes=67043328),
        name="step",
    )(starts, owned, probe_wave, fresnel_cols, fresnel_rows.reshape(2 * size, size), measured[0])
    return updated[None]


def solution(mesh):
    split = Mesh(
        mesh.devices.reshape(mesh.shape["cuts"], mesh.shape["tile"], 4, 4),
        ("cuts", "tile", "probe_0", "probe_1"),
    )
    return jax.shard_map(
        shards,
        mesh=split,
        in_specs=(
            P(),
            P(),
            P(),
            P("cuts", None, "tile", None),
            P("tile", PROBE, None),
            P("tile", PROBE, None, None),
        ),
        out_specs=P("cuts", None, TILE_PROBE, None),
        check_vma=False,
    )
```

```python
import jax
import jax.numpy as jnp
from jax import lax
from jax.experimental import pallas as pl
from jax.experimental.pallas import tpu as pltpu
from jax.sharding import Mesh
from jax.sharding import PartitionSpec as P

MARGIN = 128
LANES = 128
HOSTED = 2
LIGHT, GRADE = 0, 1
PROBE = ("probe_0", "probe_1")
TILE_PROBE = ("tile", "probe_0", "probe_1")
MESH_ID = pl.DeviceIdType.MESH
BF = jnp.bfloat16
F32 = jnp.float32
VMEM = pltpu.VMEM


def step_kernel(
    starts, owned, probe, fresnel_cols, forward_rows, measured,
    out,
    rows_here, edge_rows, mine, swapped, gathered, slab, tall, wide, amplitude_here,
    cuts, forward_cols, adjoint_cols, adjoint_rows,
    waves, cots, wave_out, cot_out, total, middle, backs,
    pieces, grids, pre, staged, got_up, got_down, partial, pre2, staged2, got_up2, got_down2,
    final, extra,
    send_z, recv_z, send_e, recv_e,
    send_f, recv_f, send_b, recv_b, send_w, recv_w,
    send_r, recv_r, send_m, recv_m, send_p, recv_p, local_sem,
):
    tile = lax.axis_index("tile")
    where = {"probe_0": lax.axis_index("probe_0"), "probe_1": lax.axis_index("probe_1")}
    sizes = {"probe_0": lax.axis_size("probe_0"), "probe_1": lax.axis_size("probe_1")}
    nx, ny = sizes["probe_0"], sizes["probe_1"]
    members = nx * ny
    spot = where["probe_0"] * ny + where["probe_1"]
    me = lax.axis_index("cuts")
    count = lax.axis_size("cuts")
    last = count - 3
    right = lax.rem(me + 1, count)
    left = lax.rem(me + count - 1, count)
    _, positions, chunks, size, pair = cuts.shape
    half = pair // 2
    hosted = 1 + me // (last - 1)
    owner_slot = HOSTED * (me // last)
    _, rows, width = owned.shape
    share = mine.shape[1]
    own = rows // members
    each = own + share
    lanes_side = width // 2

    def plane_peer(step):
        other = lax.rem(spot + step, members)
        return {"probe_0": other // ny, "probe_1": lax.rem(other, ny)}

    def across(index):
        return {"tile": 1 - tile, "probe_0": index // ny, "probe_1": lax.rem(index, ny)}

    lower = spot // (members // 2)
    edge_first = (1 - lower) * (rows - MARGIN + spot * share) + lower * (spot - members // 2) * share
    target = (1 - lower) * (members - members // 4 + spot // 2) + lower * ((spot - members // 2) // 2)
    at_end = where["probe_0"] // (nx - 1)
    at_start = (nx - 1 - where["probe_0"]) // (nx - 1)
    outer = at_end + at_start
    source = at_end * (2 * (spot - members + members // 4)) + at_start * (members // 2 + 2 * spot)

    barrier = pltpu.get_barrier_semaphore()

    def greet(device_id):
        pl.semaphore_signal(barrier, inc=1, device_id=device_id, device_id_type=MESH_ID)

    greet({"tile": 1 - tile})
    for step in range(1, members):
        greet(plane_peer(step))
    for other in (left, right):
        greet({"cuts": other})

    @pl.when(me == last)
    def _():
        greet({"cuts": count - 1})

    @pl.when(me == count - 1)
    def _():
        greet({"cuts": last})

    @pl.when(outer == 1)
    def _():
        for which in range(2):
            greet(across(source + which))

    fetch_edge = pltpu.make_async_copy(
        owned.at[:, pl.ds(pl.multiple_of(edge_first, share), share), :], edge_rows, local_sem.at[0]
    )
    fetch_edge.start()
    fetch_rows = pltpu.make_async_copy(
        owned.at[:, pl.ds(pl.multiple_of(spot * own, own), own), :], rows_here, local_sem.at[1]
    )
    fetch_rows.start()

    def fetch_slab(part):
        return pltpu.make_async_copy(owned.at[part], total.at[:, pl.ds(0, width)], local_sem.at[2])

    fetch_slab(0).start()

    def fetch_measured():
        return pltpu.make_async_copy(measured, amplitude_here, local_sem.at[3])

    @pl.when(me == last)
    def _():
        fetch_measured().start()

    fetch_edge.wait()
    mine[...] = edge_rows[...].astype(BF)
    pl.semaphore_wait(barrier, members + 3 + (me + 1) // count + (me // last) * (1 - me // (last + 1)))

    swap = pltpu.make_async_remote_copy(
        src_ref=mine, dst_ref=swapped, send_sem=send_z, recv_sem=recv_z, device_id={"tile": 1 - tile}, device_id_type=MESH_ID
    )
    @pl.when(me == 0)
    def _():
        swap.start()

    first_half, second_half = slice(0, half), slice(half, pair)

    @pl.when(me == 0)
    def _():
        for position in range(positions):
            for chunk in range(chunks):
                lanes = slice(chunk * half, (chunk + 1) * half)
                waves[0, position, chunk, :, first_half] = probe[0, :, lanes]
                waves[0, position, chunk, :, second_half] = probe[1, :, lanes]

    def turned(value):
        return value.astype(F32).T.astype(BF)

    def prepare_forward(chunk, carry):
        lanes = pl.ds(pl.multiple_of(chunk * half, half), half)
        for other in range(chunks):
            lines = slice(other * half, (other + 1) * half)
            real, imag = turned(fresnel_cols[0, lines, lanes]), turned(fresnel_cols[1, lines, lanes])
            left_lanes = slice(other * pair, other * pair + half)
            right_lanes = slice(other * pair + half, (other + 1) * pair)
            forward_cols[chunk, first_half, left_lanes] = real
            forward_cols[chunk, first_half, right_lanes] = imag
            forward_cols[chunk, second_half, left_lanes] = -imag
            forward_cols[chunk, second_half, right_lanes] = real
        return carry

    def prepare_adjoint(chunk, carry):
        lines = pl.ds(pl.multiple_of(chunk * half, half), half)
        for other in range(chunks):
            lanes = slice(other * half, (other + 1) * half)
            real, imag = fresnel_cols[0, lines, lanes], fresnel_cols[1, lines, lanes]
            left_lanes = slice(other * pair, other * pair + half)
            right_lanes = slice(other * pair + half, (other + 1) * pair)
            adjoint_cols[chunk, first_half, left_lanes] = real
            adjoint_cols[chunk, first_half, right_lanes] = -imag
            adjoint_cols[chunk, second_half, left_lanes] = imag
            adjoint_cols[chunk, second_half, right_lanes] = real
            for part in range(2):
                block = forward_rows[pl.ds(pl.multiple_of(part * size + chunk * half, half), half), lanes]
                adjoint_rows[part * size + other * half : part * size + (other + 1) * half, lines] = turned(block)
        return carry


    for part in range(2):
        fetch_slab(part).wait()
        slab[part, MARGIN : MARGIN + rows, :] = total[:, :width].astype(BF)
        if part == 0:
            fetch_slab(1).start()

    def edge_copy(step, slot):
        return pltpu.make_async_remote_copy(
            src_ref=swapped,
            dst_ref=gathered.at[slot],
            send_sem=send_e.at[step],
            recv_sem=recv_e.at[slot],
            device_id=plane_peer(step),
            device_id_type=MESH_ID,
        )

    def select(index, carry):
        position, which = index // 2, lax.rem(index, 2)
        start = starts[position, which]
        far = lax.broadcasted_iota(jnp.int32, (width, size), 0) - lax.broadcasted_iota(jnp.int32, (width, size), 1)
        tall[position, which] = jnp.where(far == start, 1.0, 0.0).astype(BF)
        far = lax.broadcasted_iota(jnp.int32, (size, width), 1) - lax.broadcasted_iota(jnp.int32, (size, width), 0)
        wide[position, which] = jnp.where(far == start, 1.0, 0.0).astype(BF)
        return carry

    def share_edges():
        swap.wait_recv()
        for step in range(1, members):
            edge_copy(step, spot).start()

    @pl.when(me > 0)
    def _():
        swap.start()

    @pl.when(me == 0)
    def _():
        share_edges()

    lax.fori_loop(0, 2 * positions, select, 0)
    lax.fori_loop(0, chunks, prepare_forward, 0)

    @pl.when(me > 0)
    def _():
        share_edges()
        lax.fori_loop(0, chunks, prepare_adjoint, 0)

    gathered[spot] = swapped[...]
    for step in range(1, members):
        edge_copy(step, lax.rem(spot + members - step, members)).wait_recv()
    for index in range(members):
        first = index * share + (rows if index >= members // 2 else 0)
        slab[:, first : first + share, :] = gathered[index]

    def cut_window(position):
        def columns(index, carry):
            part, where_to = index // 2, lax.rem(index, 2)
            lanes = pl.ds(pl.multiple_of(where_to * pair, pair), pair)
            values = jnp.dot(slab[part], tall[position, 1, :, lanes], preferred_element_type=F32).astype(BF)
            values = jnp.dot(wide[position, 0], values, preferred_element_type=F32).astype(BF)
            here = pl.ds(pl.multiple_of(part * half, half), half)
            wave_out[position, 2 * where_to, :, here] = values[:, :half]
            wave_out[position, 2 * where_to + 1, :, here] = values[:, half:]
            return carry

        lax.fori_loop(0, 4, columns, 0)

    def window_copy(position, slot, to):
        return pltpu.make_async_remote_copy(
            src_ref=wave_out.at[position],
            dst_ref=cuts.at[slot, position],
            send_sem=send_w.at[position],
            recv_sem=recv_w.at[slot, position],
            device_id={"cuts": to},
            device_id_type=MESH_ID,
        )

    give_slot = 1 - lax.rem(me + 1, 2) * (me // (last + 1))
    give_to = last - 1 + me // (last + 1)

    @pl.when(me >= last)
    def _():
        for position in range(positions):
            cut_window(position)
            window_copy(position, give_slot, give_to).start()

    @pl.when(me == last)
    def _():
        fetch_measured().wait()

    def forward_copy(position, chunk):
        return pltpu.make_async_remote_copy(
            src_ref=wave_out.at[position, chunk],
            dst_ref=waves.at[0, position, chunk],
            send_sem=send_f.at[position, chunk],
            recv_sem=recv_f.at[position, chunk],
            device_id={"cuts": right},
            device_id_type=MESH_ID,
        )

    def adjoint_copy(position, chunk):
        return pltpu.make_async_remote_copy(
            src_ref=cot_out.at[position, chunk],
            dst_ref=cots.at[position, chunk],
            send_sem=send_b.at[position, chunk],
            recv_sem=recv_b.at[position, chunk],
            device_id={"cuts": left},
            device_id_type=MESH_ID,
        )

    def parts_of(value):
        value = value.astype(F32)
        return value[:, :half], value[:, half:]

    def both(real, imag):
        return jnp.concatenate([real, imag], axis=1)

    def add_product(chunk, value, matrix):
        product = jnp.dot(value, matrix, preferred_element_type=F32)
        if chunk == 0:
            total[...] = product
        elif chunk < chunks - 1:
            total[...] += product
        else:
            product = (total[...] + product).astype(BF)
            for other in range(chunks):
                middle[other] = product[:, other * pair : (other + 1) * pair]

    def owner_copy(kind, slot, position):
        parts = pl.ds(2, 1) if kind == LIGHT else pl.ds(0, 2)
        return pltpu.make_async_remote_copy(
            src_ref=pieces.at[slot, position, parts],
            dst_ref=pieces.at[HOSTED, position, parts],
            send_sem=send_p.at[slot, position, kind],
            recv_sem=recv_p.at[position, kind],
            device_id={"cuts": lax.rem(me + 1 + slot * (me - last + 1), count)},
            device_id_type=MESH_ID,
        )

    def send_to_owner(kind, slot, position):
        @pl.when((me == last) | (slot > 0))
        def _():
            owner_copy(kind, slot, position).start()

    def forward(position):
        @pl.when(me < last)
        def _():
            cut_window(position)
            cuts[0, position] = wave_out[position]

        def hosted_slice(slot, carry):
            @pl.when((me >= last) | (slot > 0))
            def _():
                window_copy(position, slot, give_to).wait_recv()

            for chunk in range(chunks):
                @pl.when((me > 0) & (slot == 0))
                def _():
                    forward_copy(position, chunk).wait_recv()

                wave_r, wave_i = parts_of(waves[slot, position, chunk])
                win_r, win_i = parts_of(cuts[slot, position, chunk])
                out = both(wave_r * win_r - wave_i * win_i, wave_r * win_i + wave_i * win_r).astype(BF)
                add_product(chunk, out, forward_cols[chunk])

            def produce(chunk, inner):
                result = jnp.dot(forward_rows[...], middle[chunk], preferred_element_type=F32)
                real = result[:size, :half] - result[size:, half:]
                imag = result[size:, :half] + result[:size, half:]
                value = both(real, imag).astype(BF)

                @pl.when(slot < hosted - 1)
                def _():
                    waves[1, position, chunk] = value

                @pl.when(slot == hosted - 1)
                def _():
                    @pl.when(me < last)
                    def _():
                        wave_out[position, chunk] = value
                        forward_copy(position, chunk).start()

                    @pl.when(me == last)
                    def _():
                        psi_r, psi_i = parts_of(value)
                        amplitude = amplitude_here[position, :, pl.ds(pl.multiple_of(chunk * half, half), half)]
                        factor = 1.0 - amplitude * lax.rsqrt(psi_r * psi_r + psi_i * psi_i + 1.0)
                        cots[position, chunk] = both(psi_r * factor, psi_i * factor).astype(BF)

                return inner

            lax.fori_loop(0, chunks, produce, 0)

            def brighten(chunk, inner):
                wave_r, wave_i = parts_of(waves[slot, position, chunk])
                lanes = pl.ds(pl.multiple_of(chunk * half, half), half)
                pieces[slot, position, 2, :, lanes] = (wave_r * wave_r + wave_i * wave_i).astype(BF)
                return inner

            lax.fori_loop(0, chunks, brighten, 0)
            send_to_owner(LIGHT, slot, position)
            return carry

        lax.fori_loop(0, hosted, hosted_slice, 0)

    def adjoint(position):
        def hosted_slice(step, carry):
            slot = hosted - 1 - step
            for chunk in range(chunks):
                @pl.when((me < last) & (step == 0))
                def _():
                    adjoint_copy(position, chunk).wait_recv()

                add_product(chunk, cots[position, chunk], adjoint_cols[chunk])

            def produce(chunk, inner):
                result = jnp.dot(adjoint_rows[...], middle[chunk], preferred_element_type=F32)
                real = result[:size, :half] + result[size:, half:]
                imag = result[:size, half:] - result[size:, :half]
                back = both(real, imag).astype(BF)
                backs[chunk] = back

                @pl.when(me > 0)
                def _():
                    back_r, back_i = parts_of(back)
                    win_r, win_i = parts_of(cuts[slot, position, chunk])
                    value = both(win_r * back_r + win_i * back_i, win_r * back_i - win_i * back_r).astype(BF)

                    @pl.when(slot > 0)
                    def _():
                        cots[position, chunk] = value

                    @pl.when(slot == 0)
                    def _():
                        cot_out[position, chunk] = value
                        adjoint_copy(position, chunk).start()

                return inner

            lax.fori_loop(0, chunks, produce, 0)

            def grade(chunk, inner):
                wave_r, wave_i = parts_of(waves[slot, position, chunk])
                back_r, back_i = parts_of(backs[chunk])
                lanes = pl.ds(pl.multiple_of(chunk * half, half), half)
                pieces[slot, position, 0, :, lanes] = (wave_r * back_r + wave_i * back_i).astype(BF)
                pieces[slot, position, 1, :, lanes] = (wave_r * back_i - wave_i * back_r).astype(BF)
                return inner

            lax.fori_loop(0, chunks, grade, 0)
            send_to_owner(GRADE, slot, position)
            return carry

        lax.fori_loop(0, hosted, hosted_slice, 0)


    def place(part, position):
        for side in range(2):
            lanes = slice(side * lanes_side, (side + 1) * lanes_side)
            values = jnp.dot(pieces[owner_slot, position, part], wide[position, 1, :, lanes], preferred_element_type=F32)
            values = jnp.dot(tall[position, 0], values.astype(BF), preferred_element_type=F32)

            def put(add):
                for x in range(nx):
                    for y in range(ny):
                        index = x * ny + y
                        major, minor = (x, y) if side == 0 else (y, x)
                        first = MARGIN + index * own
                        second = index * share + (rows if 2 * index >= members else 0)
                        for at, depth, begins in ((0, own, first), (own, share, second)):
                            there = (side, major, part * ny + minor, pl.ds(at, depth))
                            piece = values[begins : begins + depth]
                            if add:
                                piece = piece + grids[there].astype(F32)
                            grids[there] = piece.astype(BF)

            @pl.when(position == 0)
            def _():
                put(False)

            @pl.when(position > 0)
            def _():
                put(True)

    order = (("probe_0", "probe_1"), ("probe_1", "probe_0"))
    parts_in = {LIGHT: (2,), GRADE: (0, 1)}

    def regions(kind, stage):
        parts = parts_in[kind]
        depth = len(parts) * (ny if stage == 0 else 1)
        first = parts[0] * (ny if stage == 0 else 1)
        if depth == 1:
            cut = each // 3 * 2
            return (pl.ds(first, 1), pl.ds(0, cut)), (pl.ds(first, 1), pl.ds(cut, each - cut))
        cut = depth // 2
        return (pl.ds(first, cut), pl.ds(0, each)), (pl.ds(first + cut, depth - cut), pl.ds(0, each))

    def buffers(stage, side):
        if stage == 0:
            return grids.at[side], tuple(ref.at[side] for ref in (pre, staged, got_up, got_down))
        return partial.at[side], tuple(ref.at[side] for ref in (pre2, staged2, got_up2, got_down2))

    def ring(kind, stage, side):
        axis = order[side][stage]
        length = sizes[axis]
        here = where[axis]
        plus, minus = lax.rem(here + 1, length), lax.rem(here + length - 1, length)
        opposite = lax.rem(here + 2, length)
        src, (before, queued, up, down) = buffers(stage, side)
        low, high = regions(kind, stage)

        def copy(index, source_ref, target_ref, to):
            return pltpu.make_async_remote_copy(
                src_ref=source_ref,
                dst_ref=target_ref,
                send_sem=send_r.at[kind, stage, side, index],
                recv_sem=recv_r.at[kind, stage, side, index],
                device_id={axis: to},
                device_id_type=MESH_ID,
            )

        def make(index):
            if index == 0:
                return copy(0, src.at[(opposite, *low)], before.at[low], plus)
            if index == 1:
                return copy(1, src.at[(opposite, *high)], before.at[high], minus)
            if index == 2:
                return copy(2, src.at[(plus, *high)], up.at[high], plus)
            if index == 3:
                return copy(3, src.at[(minus, *low)], down.at[low], minus)
            if index == 4:
                return copy(4, queued.at[low], up.at[low], plus)
            return copy(5, queued.at[high], down.at[high], minus)

        return make, here, plus, minus, low, high

    def begin(kind, stage, side):
        make = ring(kind, stage, side)[0]
        for index in range(4):
            make(index).start()

    def relay(kind, stage, side):
        make, _, plus, minus, low, high = ring(kind, stage, side)
        src, (before, queued, _, _) = buffers(stage, side)
        make(0).wait_recv()
        queued[low] = (before[low].astype(F32) + src[(plus, *low)].astype(F32)).astype(BF)
        make(4).start()
        make(1).wait_recv()
        queued[high] = (before[high].astype(F32) + src[(minus, *high)].astype(F32)).astype(BF)
        make(5).start()

    def settle(kind, stage, side):
        make, here, _, _, _, _ = ring(kind, stage, side)
        src, (_, _, up, down) = buffers(stage, side)
        for index in range(2, 6):
            make(index).wait_recv()
        for part in parts_in[kind]:
            if stage == 0:
                for minor in range(ny):
                    index = part * ny + minor
                    summed = src[here, index].astype(F32) + up[index].astype(F32) + down[index].astype(F32)
                    partial[side, minor, part] = summed.astype(BF)
            else:
                summed = src[here, part].astype(F32) + up[part].astype(F32) + down[part].astype(F32)
                final[side, part] = summed.astype(BF)

    def drain(kind, stage, side):
        make = ring(kind, stage, side)[0]
        for index in range(6):
            make(index).wait_send()

    def both_sides(function, kind, stage):
        for side in range(2):
            function(kind, stage, side)

    def scatter(kind):
        for stage in range(2):
            for function in (begin, relay, settle):
                both_sides(function, kind, stage)

    early = me < last - 1
    late = me // last

    @pl.when(me <= last)
    def _():
        def phase(step, carry):
            is_back = late * (step % positions) + (1 - late) * (step // positions)
            position = late * (step // positions) + (1 - late) * (step % positions)

            @pl.when((me == 0) & (step == positions))
            def _():
                lax.fori_loop(0, chunks, prepare_adjoint, 0)

            @pl.when(is_back == 0)
            def _():
                forward(position)

            @pl.when(is_back == 1)
            def _():
                adjoint(position)

            @pl.when(early)
            def _():
                def one_part(index, inner):
                    place(2 * (1 - is_back) + index, position)
                    return inner

                lax.fori_loop(0, 1 + is_back, one_part, 0)

            @pl.when(early & (step == positions - 1))
            def _():
                scatter(LIGHT)

            return carry

        lax.fori_loop(0, 2 * positions, phase, 0)

    def landed(kind, position):
        @pl.when(me >= last)
        def _():
            owner_copy(kind, 0, position).wait_recv()

    @pl.when(me >= last - 1)
    def _():
        for position in range(positions):
            landed(LIGHT, position)

        def lights_in(position, carry):
            place(2, position)
            return carry

        lax.fori_loop(0, positions, lights_in, 0)
        scatter(LIGHT)

        def grades_in(index, carry):
            position, part = index // 2, lax.rem(index, 2)

            @pl.when(part == 0)
            def _():
                landed(GRADE, position)

            place(part, position)
            return carry

        lax.fori_loop(0, 2 * positions, grades_in, 0)

    scatter(GRADE)

    def margin_copy(piece):
        return pltpu.make_async_remote_copy(
            src_ref=final.at[:, :, pl.ds(own, share), :],
            dst_ref=extra.at[piece],
            send_sem=send_m,
            recv_sem=recv_m.at[piece],
            device_id=across(target),
            device_id_type=MESH_ID,
        )

    margin_copy(lax.rem(spot, 2)).start()

    @pl.when(outer == 0)
    def _():
        extra[...] = jnp.zeros(extra.shape, extra.dtype)

    fetch_rows.wait()

    @pl.when(outer == 1)
    def _():
        for piece in range(2):
            margin_copy(piece).wait_recv()

    for side in range(2):
        columns = slice(side * lanes_side, (side + 1) * lanes_side)
        for piece in range(2):
            lines = slice(piece * share, (piece + 1) * share)
            full = final[side, :, lines, :].astype(F32) + extra[piece, side].astype(F32)
            scale = 1.0 / (full[2] + 1.0)
            for part in range(2):
                out[part, lines, columns] = rows_here[part, lines, columns] - full[part] * scale

    swap.wait_send()
    for step in range(1, members):
        edge_copy(step, spot).wait_send()

    def finish(index, carry):
        position = index // chunks
        chunk = index % chunks

        @pl.when(me < last)
        def _():
            forward_copy(position, chunk).wait_send()

        @pl.when((me > 0) & (me <= last))
        def _():
            adjoint_copy(position, chunk).wait_send()

        return carry

    lax.fori_loop(0, positions * chunks, finish, 0)

    @pl.when(me >= last)
    def _():
        for position in range(positions):
            window_copy(position, give_slot, give_to).wait_send()

    for kind in (LIGHT, GRADE):
        for stage in range(2):
            both_sides(drain, kind, stage)

    margin_copy(lax.rem(spot, 2)).wait_send()

    for slot in range(HOSTED):
        @pl.when((me == last) | ((me == last - 1) & (slot > 0)))
        def _():
            for position in range(positions):
                for kind in (LIGHT, GRADE):
                    owner_copy(kind, slot, position).wait_send()


def shards(probe_wave, fresnel_rows, fresnel_cols, object_slices, offsets, measured):
    owned = object_slices[0]
    starts = offsets[0]
    size = probe_wave.shape[1]
    positions = starts.shape[0]
    rows, width = owned.shape[1:]
    chunks = size // LANES
    pair = 2 * LANES
    nx, ny = lax.axis_size("probe_0"), lax.axis_size("probe_1")
    count = nx * ny
    share = 2 * MARGIN // count
    own = rows // count
    each = own + share
    lanes = width // 2
    dma = pltpu.SemaphoreType.DMA
    stack = (positions, chunks, size, pair)
    block = (2, 3 * ny, each, lanes)
    small = (2, 3, each, lanes)
    flags = (positions, chunks)
    anywhere = pl.BlockSpec(memory_space=pl.ANY)
    vmem = pl.BlockSpec(memory_space=pltpu.VMEM)

    updated = pl.pallas_call(
        step_kernel,
        out_shape=jax.ShapeDtypeStruct((2, own, width), F32),
        in_specs=[pl.BlockSpec(memory_space=pltpu.SMEM), anywhere, vmem, vmem, vmem, anywhere],
        out_specs=vmem,
        scratch_shapes=[
            VMEM((2, own, width), F32),
            VMEM((2, share, width), F32),
            VMEM((2, share, width), BF),
            VMEM((2, share, width), BF),
            VMEM((count, 2, share, width), BF),
            VMEM((2, rows + 2 * MARGIN, width), BF),
            VMEM((positions, 2, width, size), BF),
            VMEM((positions, 2, size, width), BF),
            VMEM((positions, size, size), F32),
            VMEM((HOSTED, *stack), BF),
            VMEM((chunks, pair, 2 * size), BF),
            VMEM((chunks, pair, 2 * size), BF),
            VMEM((2 * size, size), BF),
            VMEM((HOSTED, *stack), BF),
            VMEM(stack, BF),
            VMEM(stack, BF),
            VMEM(stack, BF),
            VMEM((size, 2 * size), F32),
            VMEM((chunks, size, pair), BF),
            VMEM((chunks, size, pair), BF),
            VMEM((HOSTED + 1, positions, 3, size, size), BF),
            VMEM((2, nx, 3 * ny, each, lanes), BF),
            VMEM(block, BF),
            VMEM(block, BF),
            VMEM(block, BF),
            VMEM(block, BF),
            VMEM((2, ny, 3, each, lanes), BF),
            VMEM(small, BF),
            VMEM(small, BF),
            VMEM(small, BF),
            VMEM(small, BF),
            VMEM(small, BF),
            VMEM((2, 2, 3, share, lanes), BF),
            dma,
            dma,
            dma((count,)),
            dma((count,)),
            dma(flags),
            dma(flags),
            dma(flags),
            dma(flags),
            dma((positions,)),
            dma((HOSTED, positions)),
            dma((2, 2, 2, 6)),
            dma((2, 2, 2, 6)),
            dma,
            dma((2,)),
            dma((HOSTED, positions, 2)),
            dma((positions, 2)),
            dma((4,)),
        ],
        compiler_params=pltpu.CompilerParams(collective_id=0, has_side_effects=True, vmem_limit_bytes=67043328),
        name="step",
    )(starts, owned, probe_wave, fresnel_cols, fresnel_rows.reshape(2 * size, size), measured[0])
    return updated[None]


def solution(mesh):
    split = Mesh(
        mesh.devices.reshape(mesh.shape["cuts"], mesh.shape["tile"], 4, 4),
        ("cuts", "tile", "probe_0", "probe_1"),
    )
    return jax.shard_map(
        shards,
        mesh=split,
        in_specs=(
            P(),
            P(),
            P(),
            P("cuts", None, "tile", None),
            P("tile", PROBE, None),
            P("tile", PROBE, None, None),
        ),
        out_specs=P("cuts", None, TILE_PROBE, None),
        check_vma=False,
    )
```

```python
import jax
import jax.numpy as jnp
from jax import lax
from jax.experimental import pallas as pl
from jax.experimental.pallas import tpu as pltpu
from jax.sharding import Mesh
from jax.sharding import PartitionSpec as P

MARGIN = 128
LANES = 128
HOSTED = 2
LIGHT, GRADE, BORDER = 0, 1, 2
PROBE = ("probe_0", "probe_1")
TILE_PROBE = ("tile", "probe_0", "probe_1")
MESH_ID = pl.DeviceIdType.MESH
BF = jnp.bfloat16
F32 = jnp.float32
VMEM = pltpu.VMEM


def step_kernel(
    starts, owned, probe_given, cols_given, rows_given, measured,
    out,
    probe, fresnel_cols, forward_rows, rows_here, edge_rows, mine, swapped, gathered, slab, tall, wide, amplitude_here,
    cuts, forward_cols, adjoint_cols, adjoint_rows,
    waves, cots, wave_out, cot_out, total, middle, backs,
    pieces, grids, pre, staged, got_up, got_down, partial, pre2, staged2, got_up2, got_down2,
    final, extra,
    send_z, recv_z, send_e, recv_e,
    send_f, recv_f, send_b, recv_b, send_w, recv_w,
    send_r, recv_r, send_m, recv_m, send_p, recv_p, local_sem,
):
    tile = lax.axis_index("tile")
    where = {"probe_0": lax.axis_index("probe_0"), "probe_1": lax.axis_index("probe_1")}
    sizes = {"probe_0": lax.axis_size("probe_0"), "probe_1": lax.axis_size("probe_1")}
    nx, ny = sizes["probe_0"], sizes["probe_1"]
    members = nx * ny
    spot = where["probe_0"] * ny + where["probe_1"]
    me = lax.axis_index("cuts")
    count = lax.axis_size("cuts")
    last = count - 3
    right = lax.rem(me + 1, count)
    left = lax.rem(me + count - 1, count)
    _, positions, chunks, size, pair = cuts.shape
    half = pair // 2
    hosted = 1 + me // (last - 1)
    owner_slot = HOSTED * (me // last)
    _, rows, width = owned.shape
    share = mine.shape[1]
    own = rows // members
    each = own + share
    lanes_side = width // 2

    def plane_peer(step):
        other = lax.rem(spot + step, members)
        return {"probe_0": other // ny, "probe_1": lax.rem(other, ny)}

    def across(index):
        return {"tile": 1 - tile, "probe_0": index // ny, "probe_1": lax.rem(index, ny)}

    lower = spot // (members // 2)
    edge_first = (1 - lower) * (rows - MARGIN + spot * share) + lower * (spot - members // 2) * share
    target = (1 - lower) * (members - members // 4 + spot // 2) + lower * ((spot - members // 2) // 2)
    at_end = where["probe_0"] // (nx - 1)
    at_start = (nx - 1 - where["probe_0"]) // (nx - 1)
    outer = at_end + at_start
    source = at_end * (2 * (spot - members + members // 4)) + at_start * (members // 2 + 2 * spot)

    barrier = pltpu.get_barrier_semaphore()

    def greet(device_id):
        pl.semaphore_signal(barrier, inc=1, device_id=device_id, device_id_type=MESH_ID)

    greet({"tile": 1 - tile})
    for step in range(1, members):
        greet(plane_peer(step))
    for other in (left, right):
        greet({"cuts": other})

    @pl.when(me == last)
    def _():
        greet({"cuts": count - 1})

    @pl.when(me == count - 1)
    def _():
        greet({"cuts": last})

    @pl.when(outer == 1)
    def _():
        for which in range(2):
            greet(across(source + which))

    fetch_edge = pltpu.make_async_copy(
        owned.at[:, pl.ds(pl.multiple_of(edge_first, share), share), :], edge_rows, local_sem.at[0]
    )
    fetch_edge.start()
    fetch_rows = pltpu.make_async_copy(
        owned.at[:, pl.ds(pl.multiple_of(spot * own, own), own), :], rows_here, local_sem.at[1]
    )
    fetch_rows.start()

    def fetch_slab(part):
        return pltpu.make_async_copy(owned.at[part], total.at[:, pl.ds(0, width)], local_sem.at[2])

    fetch_slab(0).start()

    def fetch_given(index):
        given, here = ((probe_given, probe), (cols_given, fresnel_cols), (rows_given, forward_rows))[index]
        return pltpu.make_async_copy(given, here, local_sem.at[4 + index])

    for index in range(3):
        fetch_given(index).start()

    def fetch_measured():
        return pltpu.make_async_copy(measured, amplitude_here, local_sem.at[3])

    @pl.when(me == last)
    def _():
        fetch_measured().start()

    fetch_edge.wait()
    mine[...] = edge_rows[...].astype(BF)
    pl.semaphore_wait(barrier, members + 3 + (me + 1) // count + (me // last) * (1 - me // (last + 1)))

    swap = pltpu.make_async_remote_copy(
        src_ref=mine, dst_ref=swapped, send_sem=send_z, recv_sem=recv_z, device_id={"tile": 1 - tile}, device_id_type=MESH_ID
    )
    @pl.when((me == 0) | (me >= last))
    def _():
        swap.start()

    first_half, second_half = slice(0, half), slice(half, pair)
    for index in range(3):
        fetch_given(index).wait()

    @pl.when(me == 0)
    def _():
        for position in range(positions):
            for chunk in range(chunks):
                lanes = slice(chunk * half, (chunk + 1) * half)
                waves[0, position, chunk, :, first_half] = probe[0, :, lanes]
                waves[0, position, chunk, :, second_half] = probe[1, :, lanes]

    def turned(value):
        return value.astype(F32).T.astype(BF)

    def prepare_forward(chunk, carry):
        lanes = pl.ds(pl.multiple_of(chunk * half, half), half)
        for other in range(chunks):
            lines = slice(other * half, (other + 1) * half)
            real, imag = turned(fresnel_cols[0, lines, lanes]), turned(fresnel_cols[1, lines, lanes])
            left_lanes = slice(other * pair, other * pair + half)
            right_lanes = slice(other * pair + half, (other + 1) * pair)
            forward_cols[chunk, first_half, left_lanes] = real
            forward_cols[chunk, first_half, right_lanes] = imag
            forward_cols[chunk, second_half, left_lanes] = -imag
            forward_cols[chunk, second_half, right_lanes] = real
        return carry

    def prepare_adjoint(chunk, carry):
        lines = pl.ds(pl.multiple_of(chunk * half, half), half)
        for other in range(chunks):
            lanes = slice(other * half, (other + 1) * half)
            real, imag = fresnel_cols[0, lines, lanes], fresnel_cols[1, lines, lanes]
            left_lanes = slice(other * pair, other * pair + half)
            right_lanes = slice(other * pair + half, (other + 1) * pair)
            adjoint_cols[chunk, first_half, left_lanes] = real
            adjoint_cols[chunk, first_half, right_lanes] = -imag
            adjoint_cols[chunk, second_half, left_lanes] = imag
            adjoint_cols[chunk, second_half, right_lanes] = real
            for part in range(2):
                block = forward_rows[pl.ds(pl.multiple_of(part * size + chunk * half, half), half), lanes]
                adjoint_rows[part * size + other * half : part * size + (other + 1) * half, lines] = turned(block)
        return carry


    for part in range(2):
        fetch_slab(part).wait()
        slab[part, MARGIN : MARGIN + rows, :] = total[:, :width].astype(BF)
        if part == 0:
            fetch_slab(1).start()

    def edge_copy(step, slot):
        return pltpu.make_async_remote_copy(
            src_ref=swapped,
            dst_ref=gathered.at[slot],
            send_sem=send_e.at[step],
            recv_sem=recv_e.at[slot],
            device_id=plane_peer(step),
            device_id_type=MESH_ID,
        )

    def select(index, carry):
        position, which = index // 2, lax.rem(index, 2)
        start = starts[position, which]
        far = lax.broadcasted_iota(jnp.int32, (width, size), 0) - lax.broadcasted_iota(jnp.int32, (width, size), 1)
        tall[position, which] = jnp.where(far == start, 1.0, 0.0).astype(BF)
        far = lax.broadcasted_iota(jnp.int32, (size, width), 1) - lax.broadcasted_iota(jnp.int32, (size, width), 0)
        wide[position, which] = jnp.where(far == start, 1.0, 0.0).astype(BF)
        return carry

    def share_edges():
        swap.wait_recv()
        for step in range(1, members):
            edge_copy(step, spot).start()

    @pl.when((me > 0) & (me < last))
    def _():
        swap.start()

    @pl.when((me == 0) | (me >= last))
    def _():
        share_edges()

    lax.fori_loop(0, 2 * positions, select, 0)
    lax.fori_loop(0, chunks, prepare_forward, 0)

    @pl.when((me > 0) & (me < last))
    def _():
        share_edges()

    @pl.when(me > 0)
    def _():
        lax.fori_loop(0, chunks, prepare_adjoint, 0)

    gathered[spot] = swapped[...]
    for step in range(1, members):
        edge_copy(step, lax.rem(spot + members - step, members)).wait_recv()
    for index in range(members):
        first = index * share + (rows if index >= members // 2 else 0)
        slab[:, first : first + share, :] = gathered[index]

    def cut_window(position):
        def columns(index, carry):
            part, where_to = index // 2, lax.rem(index, 2)
            lanes = pl.ds(pl.multiple_of(where_to * pair, pair), pair)
            values = jnp.dot(slab[part], tall[position, 1, :, lanes], preferred_element_type=F32).astype(BF)
            values = jnp.dot(wide[position, 0], values, preferred_element_type=F32).astype(BF)
            here = pl.ds(pl.multiple_of(part * half, half), half)
            wave_out[position, 2 * where_to, :, here] = values[:, :half]
            wave_out[position, 2 * where_to + 1, :, here] = values[:, half:]
            return carry

        lax.fori_loop(0, 4, columns, 0)

    def window_copy(position, slot, to):
        return pltpu.make_async_remote_copy(
            src_ref=wave_out.at[position],
            dst_ref=cuts.at[slot, position],
            send_sem=send_w.at[position],
            recv_sem=recv_w.at[slot, position],
            device_id={"cuts": to},
            device_id_type=MESH_ID,
        )

    give_slot = 1 - lax.rem(me + 1, 2) * (me // (last + 1))
    give_to = last - 1 + me // (last + 1)

    @pl.when(me >= last)
    def _():
        for position in range(positions):
            cut_window(position)
            window_copy(position, give_slot, give_to).start()

    @pl.when(me == last)
    def _():
        fetch_measured().wait()

    def forward_copy(position, chunk):
        return pltpu.make_async_remote_copy(
            src_ref=wave_out.at[position, chunk],
            dst_ref=waves.at[0, position, chunk],
            send_sem=send_f.at[position, chunk],
            recv_sem=recv_f.at[position, chunk],
            device_id={"cuts": right},
            device_id_type=MESH_ID,
        )

    def adjoint_copy(position, chunk):
        return pltpu.make_async_remote_copy(
            src_ref=cot_out.at[position, chunk],
            dst_ref=cots.at[position, chunk],
            send_sem=send_b.at[position, chunk],
            recv_sem=recv_b.at[position, chunk],
            device_id={"cuts": left},
            device_id_type=MESH_ID,
        )

    def parts_of(value):
        value = value.astype(F32)
        return value[:, :half], value[:, half:]

    def both(real, imag):
        return jnp.concatenate([real, imag], axis=1)

    def add_product(chunk, value, matrix):
        product = jnp.dot(value, matrix, preferred_element_type=F32)
        if chunk == 0:
            total[...] = product
        elif chunk < chunks - 1:
            total[...] += product
        else:
            product = (total[...] + product).astype(BF)
            for other in range(chunks):
                middle[other] = product[:, other * pair : (other + 1) * pair]

    def owner_copy(kind, slot, position):
        parts = pl.ds(2, 1) if kind == LIGHT else pl.ds(0, 2)
        return pltpu.make_async_remote_copy(
            src_ref=pieces.at[slot, position, parts],
            dst_ref=pieces.at[HOSTED, position, parts],
            send_sem=send_p.at[slot, position, kind],
            recv_sem=recv_p.at[position, kind],
            device_id={"cuts": lax.rem(me + 1 + slot * (me - last + 1), count)},
            device_id_type=MESH_ID,
        )

    def send_to_owner(kind, slot, position):
        @pl.when((me == last) | (slot > 0))
        def _():
            owner_copy(kind, slot, position).start()

    def forward(position):
        @pl.when(me < last)
        def _():
            cut_window(position)
            cuts[0, position] = wave_out[position]

        def hosted_slice(slot, carry):
            @pl.when((me >= last) | (slot > 0))
            def _():
                window_copy(position, slot, give_to).wait_recv()

            for chunk in range(chunks):
                @pl.when((me > 0) & (slot == 0))
                def _():
                    forward_copy(position, chunk).wait_recv()

                wave_r, wave_i = parts_of(waves[slot, position, chunk])
                win_r, win_i = parts_of(cuts[slot, position, chunk])
                out = both(wave_r * win_r - wave_i * win_i, wave_r * win_i + wave_i * win_r).astype(BF)
                add_product(chunk, out, forward_cols[chunk])

            def produce(chunk, inner):
                result = jnp.dot(forward_rows[...], middle[chunk], preferred_element_type=F32)
                real = result[:size, :half] - result[size:, half:]
                imag = result[size:, :half] + result[:size, half:]
                value = both(real, imag).astype(BF)

                @pl.when(slot < hosted - 1)
                def _():
                    waves[1, position, chunk] = value

                @pl.when(slot == hosted - 1)
                def _():
                    @pl.when(me < last)
                    def _():
                        wave_out[position, chunk] = value
                        forward_copy(position, chunk).start()

                    @pl.when(me == last)
                    def _():
                        psi_r, psi_i = parts_of(value)
                        amplitude = amplitude_here[position, :, pl.ds(pl.multiple_of(chunk * half, half), half)]
                        factor = 1.0 - amplitude * lax.rsqrt(psi_r * psi_r + psi_i * psi_i + 1.0)
                        cots[position, chunk] = both(psi_r * factor, psi_i * factor).astype(BF)

                return inner

            lax.fori_loop(0, chunks, produce, 0)

            def brighten(chunk, inner):
                wave_r, wave_i = parts_of(waves[slot, position, chunk])
                lanes = pl.ds(pl.multiple_of(chunk * half, half), half)
                pieces[slot, position, 2, :, lanes] = (wave_r * wave_r + wave_i * wave_i).astype(BF)
                return inner

            lax.fori_loop(0, chunks, brighten, 0)
            send_to_owner(LIGHT, slot, position)
            return carry

        lax.fori_loop(0, hosted, hosted_slice, 0)

    def adjoint(position):
        def hosted_slice(step, carry):
            slot = hosted - 1 - step
            for chunk in range(chunks):
                @pl.when((me < last) & (step == 0))
                def _():
                    adjoint_copy(position, chunk).wait_recv()

                add_product(chunk, cots[position, chunk], adjoint_cols[chunk])

            def produce(chunk, inner):
                result = jnp.dot(adjoint_rows[...], middle[chunk], preferred_element_type=F32)
                real = result[:size, :half] + result[size:, half:]
                imag = result[:size, half:] - result[size:, :half]
                back = both(real, imag).astype(BF)
                backs[chunk] = back

                @pl.when(me > 0)
                def _():
                    back_r, back_i = parts_of(back)
                    win_r, win_i = parts_of(cuts[slot, position, chunk])
                    value = both(win_r * back_r + win_i * back_i, win_r * back_i - win_i * back_r).astype(BF)

                    @pl.when(slot > 0)
                    def _():
                        cots[position, chunk] = value

                    @pl.when(slot == 0)
                    def _():
                        cot_out[position, chunk] = value
                        adjoint_copy(position, chunk).start()

                return inner

            lax.fori_loop(0, chunks, produce, 0)

            def grade(chunk, inner):
                wave_r, wave_i = parts_of(waves[slot, position, chunk])
                back_r, back_i = parts_of(backs[chunk])
                lanes = pl.ds(pl.multiple_of(chunk * half, half), half)
                pieces[slot, position, 0, :, lanes] = (wave_r * back_r + wave_i * back_i).astype(BF)
                pieces[slot, position, 1, :, lanes] = (wave_r * back_i - wave_i * back_r).astype(BF)
                return inner

            lax.fori_loop(0, chunks, grade, 0)
            send_to_owner(GRADE, slot, position)
            return carry

        lax.fori_loop(0, hosted, hosted_slice, 0)


    def place(part, position):
        for side in range(2):
            lanes = slice(side * lanes_side, (side + 1) * lanes_side)
            values = jnp.dot(pieces[owner_slot, position, part], wide[position, 1, :, lanes], preferred_element_type=F32)
            values = jnp.dot(tall[position, 0], values.astype(BF), preferred_element_type=F32)

            def put(add):
                for x in range(nx):
                    for y in range(ny):
                        index = x * ny + y
                        major, minor = (x, y) if side == 0 else (y, x)
                        first = MARGIN + index * own
                        second = index * share + (rows if 2 * index >= members else 0)
                        for at, depth, begins in ((0, own, first), (own, share, second)):
                            there = (side, major, part * ny + minor, pl.ds(at, depth))
                            piece = values[begins : begins + depth]
                            if add:
                                piece = piece + grids[there].astype(F32)
                            grids[there] = piece.astype(BF)

            @pl.when(position == 0)
            def _():
                put(False)

            @pl.when(position > 0)
            def _():
                put(True)

    order = (("probe_0", "probe_1"), ("probe_1", "probe_0"))
    parts_in = {LIGHT: (2,), GRADE: (0, 1), BORDER: (0, 1)}
    rows_in = {LIGHT: (0, each), GRADE: (0, own), BORDER: (own, share)}

    def regions(kind, stage):
        parts = parts_in[kind]
        start, tall_rows = rows_in[kind]
        depth = len(parts) * (ny if stage == 0 else 1)
        first = parts[0] * (ny if stage == 0 else 1)
        if depth == 1:
            cut = tall_rows // 3 * 2
            return (pl.ds(first, 1), pl.ds(start, cut)), (pl.ds(first, 1), pl.ds(start + cut, tall_rows - cut))
        cut = depth // 2
        lines = pl.ds(start, tall_rows)
        return (pl.ds(first, cut), lines), (pl.ds(first + cut, depth - cut), lines)

    def buffers(stage, side):
        if stage == 0:
            return grids.at[side], tuple(ref.at[side] for ref in (pre, staged, got_up, got_down))
        return partial.at[side], tuple(ref.at[side] for ref in (pre2, staged2, got_up2, got_down2))

    def ring(kind, stage, side):
        axis = order[side][stage]
        length = sizes[axis]
        here = where[axis]
        plus, minus = lax.rem(here + 1, length), lax.rem(here + length - 1, length)
        opposite = lax.rem(here + 2, length)
        src, (before, queued, up, down) = buffers(stage, side)
        low, high = regions(kind, stage)

        def copy(index, source_ref, target_ref, to):
            return pltpu.make_async_remote_copy(
                src_ref=source_ref,
                dst_ref=target_ref,
                send_sem=send_r.at[kind, stage, side, index],
                recv_sem=recv_r.at[kind, stage, side, index],
                device_id={axis: to},
                device_id_type=MESH_ID,
            )

        def make(index):
            if index == 0:
                return copy(0, src.at[(opposite, *low)], before.at[low], plus)
            if index == 1:
                return copy(1, src.at[(opposite, *high)], before.at[high], minus)
            if index == 2:
                return copy(2, src.at[(plus, *high)], up.at[high], plus)
            if index == 3:
                return copy(3, src.at[(minus, *low)], down.at[low], minus)
            if index == 4:
                return copy(4, queued.at[low], up.at[low], plus)
            return copy(5, queued.at[high], down.at[high], minus)

        return make, here, plus, minus, low, high

    def begin(kind, stage, side):
        make = ring(kind, stage, side)[0]
        for index in range(4):
            make(index).start()

    def relay(kind, stage, side):
        make, _, plus, minus, low, high = ring(kind, stage, side)
        src, (before, queued, _, _) = buffers(stage, side)
        make(0).wait_recv()
        queued[low] = (before[low].astype(F32) + src[(plus, *low)].astype(F32)).astype(BF)
        make(4).start()
        make(1).wait_recv()
        queued[high] = (before[high].astype(F32) + src[(minus, *high)].astype(F32)).astype(BF)
        make(5).start()

    def settle(kind, stage, side):
        make, here, _, _, _, _ = ring(kind, stage, side)
        src, (_, _, up, down) = buffers(stage, side)
        for index in range(2, 6):
            make(index).wait_recv()
        lines = pl.ds(*rows_in[kind])
        for part in parts_in[kind]:
            for minor in range(ny if stage == 0 else 1):
                index = part * ny + minor if stage == 0 else part
                summed = src[here, index, lines].astype(F32) + up[index, lines].astype(F32)
                summed = (summed + down[index, lines].astype(F32)).astype(BF)
                if stage == 0:
                    partial[side, minor, part, lines] = summed
                else:
                    final[side, part, lines] = summed

    def drain(kind, stage, side):
        make = ring(kind, stage, side)[0]
        for index in range(6):
            make(index).wait_send()

    def both_sides(function, kind, stage):
        for side in range(2):
            function(kind, stage, side)

    def scatter(kind):
        for stage in range(2):
            for function in (begin, relay, settle):
                both_sides(function, kind, stage)

    early = me < last - 1
    late = me // last

    @pl.when(me <= last)
    def _():
        def phase(step, carry):
            is_back = late * (step % positions) + (1 - late) * (step // positions)
            position = late * (step // positions) + (1 - late) * (step % positions)

            @pl.when((me == 0) & (step == positions))
            def _():
                lax.fori_loop(0, chunks, prepare_adjoint, 0)

            @pl.when(is_back == 0)
            def _():
                forward(position)

            @pl.when(is_back == 1)
            def _():
                adjoint(position)

            @pl.when(early)
            def _():
                def one_part(index, inner):
                    place(2 * (1 - is_back) + index, position)
                    return inner

                lax.fori_loop(0, 1 + is_back, one_part, 0)

            @pl.when(early & (step == positions - 1))
            def _():
                scatter(LIGHT)

            return carry

        lax.fori_loop(0, 2 * positions, phase, 0)

    def landed(kind, position):
        @pl.when(me >= last)
        def _():
            owner_copy(kind, 0, position).wait_recv()

    @pl.when(me >= last - 1)
    def _():
        for position in range(positions):
            landed(LIGHT, position)

        def lights_in(position, carry):
            place(2, position)
            return carry

        lax.fori_loop(0, positions, lights_in, 0)
        scatter(LIGHT)

        def grades_in(index, carry):
            position, part = index // 2, lax.rem(index, 2)

            @pl.when(part == 0)
            def _():
                landed(GRADE, position)

            place(part, position)
            return carry

        lax.fori_loop(0, 2 * positions, grades_in, 0)

    def margin_copy(piece):
        return pltpu.make_async_remote_copy(
            src_ref=final.at[:, :, pl.ds(own, share), :],
            dst_ref=extra.at[piece],
            send_sem=send_m,
            recv_sem=recv_m.at[piece],
            device_id=across(target),
            device_id_type=MESH_ID,
        )

    for function in (begin, relay):
        for kind in (BORDER, GRADE):
            both_sides(function, kind, 0)
    for kind in (BORDER, GRADE):
        both_sides(settle, kind, 0)
        both_sides(begin, kind, 1)
    both_sides(relay, BORDER, 1)
    both_sides(settle, BORDER, 1)
    margin_copy(lax.rem(spot, 2)).start()
    both_sides(relay, GRADE, 1)
    both_sides(settle, GRADE, 1)

    @pl.when(outer == 0)
    def _():
        extra[...] = jnp.zeros(extra.shape, extra.dtype)

    fetch_rows.wait()

    @pl.when(outer == 1)
    def _():
        for piece in range(2):
            margin_copy(piece).wait_recv()

    for side in range(2):
        columns = slice(side * lanes_side, (side + 1) * lanes_side)
        for piece in range(2):
            lines = slice(piece * share, (piece + 1) * share)
            full = final[side, :, lines, :].astype(F32) + extra[piece, side].astype(F32)
            scale = 1.0 / (full[2] + 1.0)
            for part in range(2):
                out[part, lines, columns] = rows_here[part, lines, columns] - full[part] * scale

    swap.wait_send()
    for step in range(1, members):
        edge_copy(step, spot).wait_send()

    def finish(index, carry):
        position = index // chunks
        chunk = index % chunks

        @pl.when(me < last)
        def _():
            forward_copy(position, chunk).wait_send()

        @pl.when((me > 0) & (me <= last))
        def _():
            adjoint_copy(position, chunk).wait_send()

        return carry

    lax.fori_loop(0, positions * chunks, finish, 0)

    @pl.when(me >= last)
    def _():
        for position in range(positions):
            window_copy(position, give_slot, give_to).wait_send()

    for kind in (LIGHT, GRADE, BORDER):
        for stage in range(2):
            both_sides(drain, kind, stage)

    margin_copy(lax.rem(spot, 2)).wait_send()

    for slot in range(HOSTED):
        @pl.when((me == last) | ((me == last - 1) & (slot > 0)))
        def _():
            for position in range(positions):
                for kind in (LIGHT, GRADE):
                    owner_copy(kind, slot, position).wait_send()


def shards(probe_wave, fresnel_rows, fresnel_cols, object_slices, offsets, measured):
    owned = object_slices[0]
    starts = offsets[0]
    size = probe_wave.shape[1]
    positions = starts.shape[0]
    rows, width = owned.shape[1:]
    chunks = size // LANES
    pair = 2 * LANES
    nx, ny = lax.axis_size("probe_0"), lax.axis_size("probe_1")
    count = nx * ny
    share = 2 * MARGIN // count
    own = rows // count
    each = own + share
    lanes = width // 2
    dma = pltpu.SemaphoreType.DMA
    stack = (positions, chunks, size, pair)
    block = (2, 3 * ny, each, lanes)
    small = (2, 3, each, lanes)
    flags = (positions, chunks)
    anywhere = pl.BlockSpec(memory_space=pl.ANY)
    vmem = pl.BlockSpec(memory_space=pltpu.VMEM)

    updated = pl.pallas_call(
        step_kernel,
        out_shape=jax.ShapeDtypeStruct((2, own, width), F32),
        in_specs=[pl.BlockSpec(memory_space=pltpu.SMEM)] + [anywhere] * 5,
        out_specs=vmem,
        scratch_shapes=[
            VMEM((2, size, size), BF),
            VMEM((2, size, size), BF),
            VMEM((2 * size, size), BF),
            VMEM((2, own, width), F32),
            VMEM((2, share, width), F32),
            VMEM((2, share, width), BF),
            VMEM((2, share, width), BF),
            VMEM((count, 2, share, width), BF),
            VMEM((2, rows + 2 * MARGIN, width), BF),
            VMEM((positions, 2, width, size), BF),
            VMEM((positions, 2, size, width), BF),
            VMEM((positions, size, size), F32),
            VMEM((HOSTED, *stack), BF),
            VMEM((chunks, pair, 2 * size), BF),
            VMEM((chunks, pair, 2 * size), BF),
            VMEM((2 * size, size), BF),
            VMEM((HOSTED, *stack), BF),
            VMEM(stack, BF),
            VMEM(stack, BF),
            VMEM(stack, BF),
            VMEM((size, 2 * size), F32),
            VMEM((chunks, size, pair), BF),
            VMEM((chunks, size, pair), BF),
            VMEM((HOSTED + 1, positions, 3, size, size), BF),
            VMEM((2, nx, 3 * ny, each, lanes), BF),
            VMEM(block, BF),
            VMEM(block, BF),
            VMEM(block, BF),
            VMEM(block, BF),
            VMEM((2, ny, 3, each, lanes), BF),
            VMEM(small, BF),
            VMEM(small, BF),
            VMEM(small, BF),
            VMEM(small, BF),
            VMEM(small, BF),
            VMEM((2, 2, 3, share, lanes), BF),
            dma,
            dma,
            dma((count,)),
            dma((count,)),
            dma(flags),
            dma(flags),
            dma(flags),
            dma(flags),
            dma((positions,)),
            dma((HOSTED, positions)),
            dma((3, 2, 2, 6)),
            dma((3, 2, 2, 6)),
            dma,
            dma((2,)),
            dma((HOSTED, positions, 2)),
            dma((positions, 2)),
            dma((7,)),
        ],
        compiler_params=pltpu.CompilerParams(collective_id=0, has_side_effects=True, vmem_limit_bytes=67043328),
        name="step",
    )(starts, owned, probe_wave, fresnel_cols, fresnel_rows.reshape(2 * size, size), measured[0])
    return updated[None]


def solution(mesh):
    split = Mesh(
        mesh.devices.reshape(mesh.shape["cuts"], mesh.shape["tile"], 4, 4),
        ("cuts", "tile", "probe_0", "probe_1"),
    )
    return jax.shard_map(
        shards,
        mesh=split,
        in_specs=(
            P(),
            P(),
            P(),
            P("cuts", None, "tile", None),
            P("tile", PROBE, None),
            P("tile", PROBE, None, None),
        ),
        out_specs=P("cuts", None, TILE_PROBE, None),
        check_vma=False,
    )
```

```python
import jax
import jax.numpy as jnp
from jax import lax
from jax.experimental import pallas as pl
from jax.experimental.pallas import tpu as pltpu
from jax.sharding import Mesh
from jax.sharding import PartitionSpec as P

MARGIN = 128
LANES = 128
HOSTED = 2
LIGHT, GRADE, BORDER = 0, 1, 2
PROBE = ("probe_0", "probe_1")
TILE_PROBE = ("tile", "probe_0", "probe_1")
MESH_ID = pl.DeviceIdType.MESH
BF = jnp.bfloat16
F32 = jnp.float32
VMEM = pltpu.VMEM


def step_kernel(
    starts, owned, probe_given, cols_given, rows_given, measured,
    out,
    fresnel_cols, forward_rows, rows_here, edge_rows, mine, swapped, gathered, slab, tall, wide, amplitude_here,
    cuts, forward_cols, adjoint_cols, adjoint_rows,
    waves, cots, wave_out, cot_out, total, middle, lent_backs,
    pieces, grids, pre, staged, got_up, got_down, partial, pre2, staged2, got_up2, got_down2,
    final, extra,
    send_z, recv_z, send_e, recv_e,
    send_f, recv_f, send_b, recv_b, send_w, recv_w,
    send_r, recv_r, send_m, recv_m, send_p, recv_p, send_g, recv_g, local_sem,
):
    tile = lax.axis_index("tile")
    where = {"probe_0": lax.axis_index("probe_0"), "probe_1": lax.axis_index("probe_1")}
    sizes = {"probe_0": lax.axis_size("probe_0"), "probe_1": lax.axis_size("probe_1")}
    nx, ny = sizes["probe_0"], sizes["probe_1"]
    members = nx * ny
    spot = where["probe_0"] * ny + where["probe_1"]
    me = lax.axis_index("cuts")
    count = lax.axis_size("cuts")
    last = count - 3
    right = lax.rem(me + 1, count)
    left = lax.rem(me + count - 1, count)
    _, positions, chunks, size, pair = cuts.shape
    half = pair // 2
    hosted = 1 + me // (last - 1)
    host = last - 1
    lender = (me == host - 1) | (me == host - 2)
    extra_slots = 2 * (me // host) * (1 - me // last)
    before = left - 2 * (me // host) * (1 - me // last)
    owner_slot = HOSTED * (me // last)
    _, rows, width = owned.shape
    share = mine.shape[1]
    own = rows // members
    each = own + share
    lanes_side = width // 2

    def plane_peer(step):
        other = lax.rem(spot + step, members)
        return {"probe_0": other // ny, "probe_1": lax.rem(other, ny)}

    def across(index):
        return {"tile": 1 - tile, "probe_0": index // ny, "probe_1": lax.rem(index, ny)}

    lower = spot // (members // 2)
    edge_first = (1 - lower) * (rows - MARGIN + spot * share) + lower * (spot - members // 2) * share
    target = (1 - lower) * (members - members // 4 + spot // 2) + lower * ((spot - members // 2) // 2)
    at_end = where["probe_0"] // (nx - 1)
    at_start = (nx - 1 - where["probe_0"]) // (nx - 1)
    outer = at_end + at_start
    source = at_end * (2 * (spot - members + members // 4)) + at_start * (members // 2 + 2 * spot)

    barrier = pltpu.get_barrier_semaphore()

    def greet(device_id):
        pl.semaphore_signal(barrier, inc=1, device_id=device_id, device_id_type=MESH_ID)

    greet({"tile": 1 - tile})
    for step in range(1, members):
        greet(plane_peer(step))
    for other in (left, right):
        greet({"cuts": other})

    @pl.when(me == last)
    def _():
        greet({"cuts": count - 1})

    @pl.when(me == count - 1)
    def _():
        greet({"cuts": last})

    @pl.when((me == host - 2) | (me == host - 3))
    def _():
        greet({"cuts": host})

    @pl.when(me == host)
    def _():
        for step in (2, 3):
            greet({"cuts": host - step})

    @pl.when(outer == 1)
    def _():
        for which in range(2):
            greet(across(source + which))

    fetch_edge = pltpu.make_async_copy(
        owned.at[:, pl.ds(pl.multiple_of(edge_first, share), share), :], edge_rows, local_sem.at[0]
    )
    fetch_edge.start()
    fetch_rows = pltpu.make_async_copy(
        owned.at[:, pl.ds(pl.multiple_of(spot * own, own), own), :], rows_here, local_sem.at[1]
    )
    fetch_rows.start()

    def fetch_slab(part):
        return pltpu.make_async_copy(owned.at[part], total.at[:, pl.ds(0, width)], local_sem.at[2])

    fetch_slab(0).start()

    def fetch_given(index):
        given, here = ((probe_given, pieces.at[0, 0, pl.ds(0, 2)]), (cols_given, fresnel_cols), (rows_given, forward_rows))[index]
        return pltpu.make_async_copy(given, here, local_sem.at[4 + index])

    for index in range(3):
        fetch_given(index).start()

    def fetch_measured(position):
        return pltpu.make_async_copy(measured.at[position], amplitude_here, local_sem.at[3])

    fetch_edge.wait()
    mine[...] = edge_rows[...].astype(BF)
    one_more = (me == last) | (me == count - 1) | (me == host - 2) | (me == host - 3)

    @pl.when(me == host)
    def _():
        pl.semaphore_wait(barrier, members + 5)

    @pl.when(one_more)
    def _():
        pl.semaphore_wait(barrier, members + 4)

    @pl.when((me == 0) | (me == host - 1) | (me == last + 1))
    def _():
        pl.semaphore_wait(barrier, members + 3)

    swap = pltpu.make_async_remote_copy(
        src_ref=mine, dst_ref=swapped, send_sem=send_z, recv_sem=recv_z, device_id={"tile": 1 - tile}, device_id_type=MESH_ID
    )
    @pl.when((me == 0) | (me >= last))
    def _():
        swap.start()

    first_half, second_half = slice(0, half), slice(half, pair)
    for index in range(3):
        fetch_given(index).wait()

    @pl.when(me == 0)
    def _():
        for position in range(positions):
            for chunk in range(chunks):
                lanes = slice(chunk * half, (chunk + 1) * half)
                waves[0, position, chunk, :, first_half] = pieces[0, 0, 0, :, lanes]
                waves[0, position, chunk, :, second_half] = pieces[0, 0, 1, :, lanes]

    def turned(value):
        return value.astype(F32).T.astype(BF)

    def prepare_forward(chunk, carry):
        lanes = pl.ds(pl.multiple_of(chunk * half, half), half)
        for other in range(chunks):
            lines = slice(other * half, (other + 1) * half)
            real, imag = turned(fresnel_cols[0, lines, lanes]), turned(fresnel_cols[1, lines, lanes])
            left_lanes = slice(other * pair, other * pair + half)
            right_lanes = slice(other * pair + half, (other + 1) * pair)
            forward_cols[chunk, first_half, left_lanes] = real
            forward_cols[chunk, first_half, right_lanes] = imag
            forward_cols[chunk, second_half, left_lanes] = -imag
            forward_cols[chunk, second_half, right_lanes] = real
        return carry

    def prepare_adjoint(chunk, carry):
        lines = pl.ds(pl.multiple_of(chunk * half, half), half)
        for other in range(chunks):
            lanes = slice(other * half, (other + 1) * half)
            real, imag = fresnel_cols[0, lines, lanes], fresnel_cols[1, lines, lanes]
            left_lanes = slice(other * pair, other * pair + half)
            right_lanes = slice(other * pair + half, (other + 1) * pair)
            adjoint_cols[chunk, first_half, left_lanes] = real
            adjoint_cols[chunk, first_half, right_lanes] = -imag
            adjoint_cols[chunk, second_half, left_lanes] = imag
            adjoint_cols[chunk, second_half, right_lanes] = real
            for part in range(2):
                block = forward_rows[pl.ds(pl.multiple_of(part * size + chunk * half, half), half), lanes]
                adjoint_rows[part * size + other * half : part * size + (other + 1) * half, lines] = turned(block)
        return carry


    for part in range(2):
        fetch_slab(part).wait()
        slab[part, MARGIN : MARGIN + rows, :] = total[:, :width].astype(BF)
        if part == 0:
            fetch_slab(1).start()

    def edge_copy(step, slot):
        return pltpu.make_async_remote_copy(
            src_ref=swapped,
            dst_ref=gathered.at[slot],
            send_sem=send_e.at[step],
            recv_sem=recv_e.at[slot],
            device_id=plane_peer(step),
            device_id_type=MESH_ID,
        )

    def select(index, carry):
        position, which = index // 2, lax.rem(index, 2)
        start = starts[position, which]
        far = lax.broadcasted_iota(jnp.int32, (width, size), 0) - lax.broadcasted_iota(jnp.int32, (width, size), 1)
        tall[position, which] = jnp.where(far == start, 1.0, 0.0).astype(BF)
        far = lax.broadcasted_iota(jnp.int32, (size, width), 1) - lax.broadcasted_iota(jnp.int32, (size, width), 0)
        wide[position, which] = jnp.where(far == start, 1.0, 0.0).astype(BF)
        return carry

    def share_edges():
        swap.wait_recv()
        for step in range(1, members):
            edge_copy(step, spot).start()

    @pl.when((me > 0) & (me < last))
    def _():
        swap.start()

    @pl.when((me == 0) | (me >= last))
    def _():
        share_edges()

    lax.fori_loop(0, 2 * positions, select, 0)
    lax.fori_loop(0, chunks, prepare_forward, 0)

    @pl.when((me > 0) & (me < last))
    def _():
        share_edges()

    @pl.when(me > 0)
    def _():
        lax.fori_loop(0, chunks, prepare_adjoint, 0)

    gathered[spot] = swapped[...]
    for step in range(1, members):
        edge_copy(step, lax.rem(spot + members - step, members)).wait_recv()
    for index in range(members):
        first = index * share + (rows if index >= members // 2 else 0)
        slab[:, first : first + share, :] = gathered[index]

    def cut_window(position):
        def columns(index, carry):
            part, where_to = index // 2, lax.rem(index, 2)
            lanes = pl.ds(pl.multiple_of(where_to * pair, pair), pair)
            values = jnp.dot(slab[part], tall[position, 1, :, lanes], preferred_element_type=F32).astype(BF)
            values = jnp.dot(wide[position, 0], values, preferred_element_type=F32).astype(BF)
            here = pl.ds(pl.multiple_of(part * half, half), half)
            wave_out[position, 2 * where_to, :, here] = values[:, :half]
            wave_out[position, 2 * where_to + 1, :, here] = values[:, half:]
            return carry

        lax.fori_loop(0, 4, columns, 0)

    def window_copy(position, slot, to):
        return pltpu.make_async_remote_copy(
            src_ref=wave_out.at[position],
            dst_ref=cuts.at[slot, position],
            send_sem=send_w.at[position],
            recv_sem=recv_w.at[slot, position],
            device_id={"cuts": to},
            device_id_type=MESH_ID,
        )

    give_slot = 1 - lax.rem(me + 1, 2) * (me // (last + 1))
    give_to = last - 1 + me // (last + 1)

    def lend(position):
        slot = HOSTED + lax.rem(me, 2)
        return pltpu.make_async_remote_copy(
            src_ref=cuts.at[0, position],
            dst_ref=cuts.at[slot, position],
            send_sem=send_w.at[position],
            recv_sem=recv_w.at[slot, position],
            device_id={"cuts": host},
            device_id_type=MESH_ID,
        )

    @pl.when(lender)
    def _():
        for position in range(positions):
            cut_window(position)
            cuts[0, position] = wave_out[position]
        lend(0).start()

    @pl.when(me >= last)
    def _():
        for position in range(positions):
            cut_window(position)
            window_copy(position, give_slot, give_to).start()

    def forward_copy(position, chunk):
        return pltpu.make_async_remote_copy(
            src_ref=wave_out.at[position, chunk],
            dst_ref=waves.at[0, position, chunk],
            send_sem=send_f.at[position, chunk],
            recv_sem=recv_f.at[position, chunk],
            device_id={"cuts": right},
            device_id_type=MESH_ID,
        )

    def adjoint_copy(position, chunk):
        return pltpu.make_async_remote_copy(
            src_ref=cot_out.at[position, chunk],
            dst_ref=cots.at[position, chunk],
            send_sem=send_b.at[position, chunk],
            recv_sem=recv_b.at[position, chunk],
            device_id={"cuts": before},
            device_id_type=MESH_ID,
        )

    def parts_of(value):
        value = value.astype(F32)
        return value[:, :half], value[:, half:]

    def both(real, imag):
        return jnp.concatenate([real, imag], axis=1)

    def add_product(chunk, value, matrix):
        product = jnp.dot(value, matrix, preferred_element_type=F32)
        if chunk == 0:
            total[...] = product
        elif chunk < chunks - 1:
            total[...] += product
        else:
            product = (total[...] + product).astype(BF)
            for other in range(chunks):
                middle[other] = product[:, other * pair : (other + 1) * pair]

    def owner_copy(kind, slot, position):
        parts = pl.ds(2, 1) if kind == LIGHT else pl.ds(0, 2)
        return pltpu.make_async_remote_copy(
            src_ref=pieces.at[slot, position, parts],
            dst_ref=pieces.at[HOSTED, position, parts],
            send_sem=send_p.at[slot, position, kind],
            recv_sem=recv_p.at[position, kind],
            device_id={"cuts": lax.rem(me + 1 + slot * (me - last + 1), count)},
            device_id_type=MESH_ID,
        )

    def send_to_owner(kind, slot, position):
        @pl.when((me == last) | (slot > 0))
        def _():
            owner_copy(kind, slot, position).start()

    def forward(position):
        @pl.when((me < host - 2) | (me == host))
        def _():
            cut_window(position)
            cuts[0, position] = wave_out[position]

        @pl.when(me == last)
        def _():
            fetch_measured(position).start()

        def hosted_slice(slot, carry):
            @pl.when((me >= last) | (slot > 0))
            def _():
                window_copy(position, slot, give_to).wait_recv()

            for chunk in range(chunks):
                @pl.when((me > 0) & (slot == 0))
                def _():
                    forward_copy(position, chunk).wait_recv()

                wave_r, wave_i = parts_of(waves[slot, position, chunk])
                win_r, win_i = parts_of(cuts[slot, position, chunk])
                out = both(wave_r * win_r - wave_i * win_i, wave_r * win_i + wave_i * win_r).astype(BF)
                add_product(chunk, out, forward_cols[chunk])

            @pl.when((me == last) & (slot == hosted - 1))
            def _():
                fetch_measured(position).wait()

            def produce(chunk, inner):
                result = jnp.dot(forward_rows[...], middle[chunk], preferred_element_type=F32)
                real = result[:size, :half] - result[size:, half:]
                imag = result[size:, :half] + result[:size, half:]
                value = both(real, imag).astype(BF)

                @pl.when(slot < hosted - 1)
                def _():
                    waves[1, position, chunk] = value

                @pl.when(slot == hosted - 1)
                def _():
                    @pl.when(me < last)
                    def _():
                        wave_out[position, chunk] = value
                        forward_copy(position, chunk).start()

                    @pl.when(me == last)
                    def _():
                        psi_r, psi_i = parts_of(value)
                        amplitude = amplitude_here[:, pl.ds(pl.multiple_of(chunk * half, half), half)]
                        factor = 1.0 - amplitude * lax.rsqrt(psi_r * psi_r + psi_i * psi_i + 1.0)
                        cots[position, chunk] = both(psi_r * factor, psi_i * factor).astype(BF)

                return inner

            lax.fori_loop(0, chunks, produce, 0)

            def brighten(chunk, inner):
                wave_r, wave_i = parts_of(waves[slot, position, chunk])
                lanes = pl.ds(pl.multiple_of(chunk * half, half), half)
                pieces[slot, position, 2, :, lanes] = (wave_r * wave_r + wave_i * wave_i).astype(BF)
                return inner

            lax.fori_loop(0, chunks, brighten, 0)
            send_to_owner(LIGHT, slot, position)
            return carry

        lax.fori_loop(0, hosted, hosted_slice, 0)

    def grade_all(position, slot):
        def grade(chunk, inner):
            wave_r, wave_i = parts_of(waves[slot, position, chunk])
            back_r, back_i = parts_of(middle[chunk])
            lanes = pl.ds(pl.multiple_of(chunk * half, half), half)
            pieces[slot, position, 0, :, lanes] = (wave_r * back_r + wave_i * back_i).astype(BF)
            pieces[slot, position, 1, :, lanes] = (wave_r * back_i - wave_i * back_r).astype(BF)
            return inner

        lax.fori_loop(0, chunks, grade, 0)

    def return_back(position, which):
        return pltpu.make_async_remote_copy(
            src_ref=lent_backs.at[which, position],
            dst_ref=cots.at[position],
            send_sem=send_g.at[which, position],
            recv_sem=recv_g.at[position],
            device_id={"cuts": host - 2 + which},
            device_id_type=MESH_ID,
        )

    def adjoint(position):
        def hosted_slice(step, carry):
            foreign = step // hosted
            slot = (hosted - 1 - step) * (1 - foreign) + (2 * HOSTED + 1 - step) * foreign

            @pl.when(foreign > 0)
            def _():
                pltpu.make_async_remote_copy(
                    src_ref=cuts.at[0, position],
                    dst_ref=cuts.at[slot, position],
                    send_sem=send_w.at[position],
                    recv_sem=recv_w.at[slot, position],
                    device_id={"cuts": host - 1},
                    device_id_type=MESH_ID,
                ).wait_recv()

            for chunk in range(chunks):
                @pl.when((me < last) & (step == 0))
                def _():
                    adjoint_copy(position, chunk).wait_recv()

                add_product(chunk, cots[position, chunk], adjoint_cols[chunk])

            def produce(chunk, inner):
                result = jnp.dot(adjoint_rows[...], middle[chunk], preferred_element_type=F32)
                real = result[:size, :half] + result[size:, half:]
                imag = result[:size, half:] - result[size:, :half]
                back = both(real, imag).astype(BF)

                @pl.when(foreign == 0)
                def _():
                    middle[chunk] = back

                @pl.when(foreign > 0)
                def _():
                    lent_backs[slot - HOSTED, position, chunk] = back

                @pl.when(me > 0)
                def _():
                    back_r, back_i = parts_of(back)
                    win_r, win_i = parts_of(cuts[slot, position, chunk])
                    value = both(win_r * back_r + win_i * back_i, win_r * back_i - win_i * back_r).astype(BF)

                    @pl.when(step < hosted + extra_slots - 1)
                    def _():
                        cots[position, chunk] = value

                    @pl.when(step == hosted + extra_slots - 1)
                    def _():
                        cot_out[position, chunk] = value
                        adjoint_copy(position, chunk).start()

                return inner

            lax.fori_loop(0, chunks, produce, 0)

            @pl.when(foreign == 0)
            def _():
                grade_all(position, lax.rem(slot, HOSTED))
                send_to_owner(GRADE, lax.rem(slot, HOSTED), position)

            return carry

        lax.fori_loop(0, hosted + extra_slots, hosted_slice, 0)


    def place(part, position):
        for side in range(2):
            lanes = slice(side * lanes_side, (side + 1) * lanes_side)
            values = jnp.dot(pieces[owner_slot, position, part], wide[position, 1, :, lanes], preferred_element_type=F32)
            values = jnp.dot(tall[position, 0], values.astype(BF), preferred_element_type=F32)

            def put(add):
                for x in range(nx):
                    for y in range(ny):
                        index = x * ny + y
                        major, minor = (x, y) if side == 0 else (y, x)
                        first = MARGIN + index * own
                        second = index * share + (rows if 2 * index >= members else 0)
                        for at, depth, begins in ((0, own, first), (own, share, second)):
                            there = (side, major, part * ny + minor, pl.ds(at, depth))
                            piece = values[begins : begins + depth]
                            if add:
                                piece = piece + grids[there].astype(F32)
                            grids[there] = piece.astype(BF)

            @pl.when(position == 0)
            def _():
                put(False)

            @pl.when(position > 0)
            def _():
                put(True)

    order = (("probe_0", "probe_1"), ("probe_1", "probe_0"))
    parts_in = {LIGHT: (2,), GRADE: (0, 1), BORDER: (0, 1)}
    rows_in = {LIGHT: (0, each), GRADE: (0, own), BORDER: (own, share)}

    def regions(kind, stage):
        parts = parts_in[kind]
        start, tall_rows = rows_in[kind]
        depth = len(parts) * (ny if stage == 0 else 1)
        first = parts[0] * (ny if stage == 0 else 1)
        if depth == 1:
            cut = tall_rows // 3 * 2
            return (pl.ds(first, 1), pl.ds(start, cut)), (pl.ds(first, 1), pl.ds(start + cut, tall_rows - cut))
        cut = depth // 2
        lines = pl.ds(start, tall_rows)
        return (pl.ds(first, cut), lines), (pl.ds(first + cut, depth - cut), lines)

    def buffers(stage, side):
        if stage == 0:
            return grids.at[side], tuple(ref.at[side] for ref in (pre, staged, got_up, got_down))
        return partial.at[side], tuple(ref.at[side] for ref in (pre2, staged2, got_up2, got_down2))

    def ring(kind, stage, side):
        axis = order[side][stage]
        length = sizes[axis]
        here = where[axis]
        plus, minus = lax.rem(here + 1, length), lax.rem(here + length - 1, length)
        opposite = lax.rem(here + 2, length)
        src, (before, queued, up, down) = buffers(stage, side)
        low, high = regions(kind, stage)

        def copy(index, source_ref, target_ref, to):
            return pltpu.make_async_remote_copy(
                src_ref=source_ref,
                dst_ref=target_ref,
                send_sem=send_r.at[kind, stage, side, index],
                recv_sem=recv_r.at[kind, stage, side, index],
                device_id={axis: to},
                device_id_type=MESH_ID,
            )

        def make(index):
            if index == 0:
                return copy(0, src.at[(opposite, *low)], before.at[low], plus)
            if index == 1:
                return copy(1, src.at[(opposite, *high)], before.at[high], minus)
            if index == 2:
                return copy(2, src.at[(plus, *high)], up.at[high], plus)
            if index == 3:
                return copy(3, src.at[(minus, *low)], down.at[low], minus)
            if index == 4:
                return copy(4, queued.at[low], up.at[low], plus)
            return copy(5, queued.at[high], down.at[high], minus)

        return make, here, plus, minus, low, high

    def begin(kind, stage, side):
        make = ring(kind, stage, side)[0]
        for index in range(4):
            make(index).start()

    def relay(kind, stage, side):
        make, _, plus, minus, low, high = ring(kind, stage, side)
        src, (before, queued, _, _) = buffers(stage, side)
        make(0).wait_recv()
        queued[low] = (before[low].astype(F32) + src[(plus, *low)].astype(F32)).astype(BF)
        make(4).start()
        make(1).wait_recv()
        queued[high] = (before[high].astype(F32) + src[(minus, *high)].astype(F32)).astype(BF)
        make(5).start()

    def settle(kind, stage, side):
        make, here, _, _, _, _ = ring(kind, stage, side)
        src, (_, _, up, down) = buffers(stage, side)
        for index in range(2, 6):
            make(index).wait_recv()
        lines = pl.ds(*rows_in[kind])
        for part in parts_in[kind]:
            for minor in range(ny if stage == 0 else 1):
                index = part * ny + minor if stage == 0 else part
                summed = src[here, index, lines].astype(F32) + up[index, lines].astype(F32)
                summed = (summed + down[index, lines].astype(F32)).astype(BF)
                if stage == 0:
                    partial[side, minor, part, lines] = summed
                else:
                    final[side, part, lines] = summed

    def drain(kind, stage, side):
        make = ring(kind, stage, side)[0]
        for index in range(6):
            make(index).wait_send()

    def both_sides(function, kind, stage):
        for side in range(2):
            function(kind, stage, side)

    def scatter(kind):
        for stage in range(2):
            for function in (begin, relay, settle):
                both_sides(function, kind, stage)

    early = me < last - 1
    late = me // last

    @pl.when(me <= last)
    def _():
        def phase(step, carry):
            is_back = late * (step % positions) + (1 - late) * (step // positions)
            position = late * (step // positions) + (1 - late) * (step % positions)

            @pl.when((me == 0) & (step == positions))
            def _():
                lax.fori_loop(0, chunks, prepare_adjoint, 0)

            @pl.when(is_back == 0)
            def _():
                forward(position)

            @pl.when((is_back == 1) & ((me < host - 2) | (me >= host)))
            def _():
                adjoint(position)

            @pl.when((is_back == 1) & lender)
            def _():
                return_back(position, 0).wait_recv()
                for chunk in range(chunks):
                    middle[chunk] = cots[position, chunk]
                grade_all(position, 0)

            @pl.when(early)
            def _():
                def one_part(index, inner):
                    place(2 * (1 - is_back) + index, position)
                    return inner

                lax.fori_loop(0, 1 + is_back, one_part, 0)

            @pl.when(lender & (step == positions - 1))
            def _():
                for late_position in range(1, positions):
                    lend(late_position).start()

            @pl.when(early & (step == positions - 1))
            def _():
                scatter(LIGHT)

            return carry

        lax.fori_loop(0, 2 * positions, phase, 0)

        @pl.when(me == host)
        def _():
            for position in range(positions):
                for which in range(2):
                    return_back(position, which).start()

    def landed(kind, position):
        @pl.when(me >= last)
        def _():
            owner_copy(kind, 0, position).wait_recv()

    @pl.when(me >= last - 1)
    def _():
        for position in range(positions):
            landed(LIGHT, position)

        def lights_in(position, carry):
            place(2, position)
            return carry

        lax.fori_loop(0, positions, lights_in, 0)
        scatter(LIGHT)

        def grades_in(index, carry):
            position, part = index // 2, lax.rem(index, 2)

            @pl.when(part == 0)
            def _():
                landed(GRADE, position)

            place(part, position)
            return carry

        lax.fori_loop(0, 2 * positions, grades_in, 0)

    def margin_copy(piece):
        return pltpu.make_async_remote_copy(
            src_ref=final.at[:, :, pl.ds(own, share), :],
            dst_ref=extra.at[piece],
            send_sem=send_m,
            recv_sem=recv_m.at[piece],
            device_id=across(target),
            device_id_type=MESH_ID,
        )

    for function in (begin, relay):
        for kind in (BORDER, GRADE):
            both_sides(function, kind, 0)
    for kind in (BORDER, GRADE):
        both_sides(settle, kind, 0)
        both_sides(begin, kind, 1)
    both_sides(relay, BORDER, 1)
    both_sides(settle, BORDER, 1)
    margin_copy(lax.rem(spot, 2)).start()
    both_sides(relay, GRADE, 1)
    both_sides(settle, GRADE, 1)

    @pl.when(outer == 0)
    def _():
        extra[...] = jnp.zeros(extra.shape, extra.dtype)

    fetch_rows.wait()

    @pl.when(outer == 1)
    def _():
        for piece in range(2):
            margin_copy(piece).wait_recv()

    for side in range(2):
        columns = slice(side * lanes_side, (side + 1) * lanes_side)
        for piece in range(2):
            lines = slice(piece * share, (piece + 1) * share)
            full = final[side, :, lines, :].astype(F32) + extra[piece, side].astype(F32)
            scale = 1.0 / (full[2] + 1.0)
            for part in range(2):
                out[part, lines, columns] = rows_here[part, lines, columns] - full[part] * scale

    swap.wait_send()
    for step in range(1, members):
        edge_copy(step, spot).wait_send()

    def finish(index, carry):
        position = index // chunks
        chunk = index % chunks

        @pl.when(me < last)
        def _():
            forward_copy(position, chunk).wait_send()

        @pl.when((me > 0) & (me <= last) & ((me < host - 2) | (me >= host)))
        def _():
            adjoint_copy(position, chunk).wait_send()

        return carry

    lax.fori_loop(0, positions * chunks, finish, 0)

    @pl.when(me >= last)
    def _():
        for position in range(positions):
            window_copy(position, give_slot, give_to).wait_send()

    @pl.when(lender)
    def _():
        for position in range(positions):
            lend(position).wait_send()

    @pl.when(me == host)
    def _():
        for position in range(positions):
            for which in range(2):
                return_back(position, which).wait_send()

    for kind in (LIGHT, GRADE, BORDER):
        for stage in range(2):
            both_sides(drain, kind, stage)

    margin_copy(lax.rem(spot, 2)).wait_send()

    for slot in range(HOSTED):
        @pl.when((me == last) | ((me == last - 1) & (slot > 0)))
        def _():
            for position in range(positions):
                for kind in (LIGHT, GRADE):
                    owner_copy(kind, slot, position).wait_send()


def shards(probe_wave, fresnel_rows, fresnel_cols, object_slices, offsets, measured):
    owned = object_slices[0]
    starts = offsets[0]
    size = probe_wave.shape[1]
    positions = starts.shape[0]
    rows, width = owned.shape[1:]
    chunks = size // LANES
    pair = 2 * LANES
    nx, ny = lax.axis_size("probe_0"), lax.axis_size("probe_1")
    count = nx * ny
    share = 2 * MARGIN // count
    own = rows // count
    each = own + share
    lanes = width // 2
    dma = pltpu.SemaphoreType.DMA
    stack = (positions, chunks, size, pair)
    block = (2, 3 * ny, each, lanes)
    small = (2, 3, each, lanes)
    flags = (positions, chunks)
    anywhere = pl.BlockSpec(memory_space=pl.ANY)
    vmem = pl.BlockSpec(memory_space=pltpu.VMEM)

    updated = pl.pallas_call(
        step_kernel,
        out_shape=jax.ShapeDtypeStruct((2, own, width), F32),
        in_specs=[pl.BlockSpec(memory_space=pltpu.SMEM)] + [anywhere] * 5,
        out_specs=vmem,
        scratch_shapes=[
            VMEM((2, size, size), BF),
            VMEM((2 * size, size), BF),
            VMEM((2, own, width), F32),
            VMEM((2, share, width), F32),
            VMEM((2, share, width), BF),
            VMEM((2, share, width), BF),
            VMEM((count, 2, share, width), BF),
            VMEM((2, rows + 2 * MARGIN, width), BF),
            VMEM((positions, 2, width, size), BF),
            VMEM((positions, 2, size, width), BF),
            VMEM((size, size), F32),
            VMEM((2 * HOSTED, *stack), BF),
            VMEM((chunks, pair, 2 * size), BF),
            VMEM((chunks, pair, 2 * size), BF),
            VMEM((2 * size, size), BF),
            VMEM((HOSTED, *stack), BF),
            VMEM(stack, BF),
            VMEM(stack, BF),
            VMEM(stack, BF),
            VMEM((size, 2 * size), F32),
            VMEM((chunks, size, pair), BF),
            VMEM((2, *stack), BF),
            VMEM((HOSTED + 1, positions, 3, size, size), BF),
            VMEM((2, nx, 3 * ny, each, lanes), BF),
            VMEM(block, BF),
            VMEM(block, BF),
            VMEM(block, BF),
            VMEM(block, BF),
            VMEM((2, ny, 3, each, lanes), BF),
            VMEM(small, BF),
            VMEM(small, BF),
            VMEM(small, BF),
            VMEM(small, BF),
            VMEM(small, BF),
            VMEM((2, 2, 3, share, lanes), BF),
            dma,
            dma,
            dma((count,)),
            dma((count,)),
            dma(flags),
            dma(flags),
            dma(flags),
            dma(flags),
            dma((positions,)),
            dma((2 * HOSTED, positions)),
            dma((3, 2, 2, 6)),
            dma((3, 2, 2, 6)),
            dma,
            dma((2,)),
            dma((HOSTED, positions, 2)),
            dma((positions, 2)),
            dma((2, positions)),
            dma((positions,)),
            dma((7,)),
        ],
        compiler_params=pltpu.CompilerParams(collective_id=0, has_side_effects=True, vmem_limit_bytes=67043328),
        name="step",
    )(starts, owned, probe_wave, fresnel_cols, fresnel_rows.reshape(2 * size, size), measured[0])
    return updated[None]


def solution(mesh):
    split = Mesh(
        mesh.devices.reshape(mesh.shape["cuts"], mesh.shape["tile"], 4, 4),
        ("cuts", "tile", "probe_0", "probe_1"),
    )
    return jax.shard_map(
        shards,
        mesh=split,
        in_specs=(
            P(),
            P(),
            P(),
            P("cuts", None, "tile", None),
            P("tile", PROBE, None),
            P("tile", PROBE, None, None),
        ),
        out_specs=P("cuts", None, TILE_PROBE, None),
        check_vma=False,
    )
```
